256 devices in a mesh: row: 16 (over y_lo, z), col: 16 (over x, y_hi, core).
Axes of the slice: x: 4, y: 4 (y_hi: 2, y_lo: 2; y = y_hi * 2 + y_lo), z: 8, core: 2. Of those that a mesh axis runs over, the one named last changes fastest.
Arguments:
- field: float32 [512, 64, 8, 512], P('row', 'col'), may hold values from -6 to 6
- modes: int32 [3, 256], replicated, may hold values from 0 to 511, as said below
Outputs:
- spectrum: float32 [64, 512, 8, 512], P(None, 'col', None, 'row')
- localized: float32 [512, 512], replicated
The draws below stay inside these ranges and needn't reach their ends.
Inputs may be any that keep to these rules, and one draw needn't show every extreme that they name: `modes`: row 0 holds kx in 0 to 255, row 1 ky in 0 to 511, row 2 kz in 0 to 63; triples may repeat.
All inputs are finite; a program needn't handle non-finite values.
Results may differ from the reference program's by a relative error of at most 0.00013.
Values sent between devices are 32-bit elements; how exact they have to be, the bound alone decides.
A program may use at most 128 MiB of HBM per device.

```python
import math
import jax
import jax.numpy as jnp
from jax import lax

NX = 512
NY = 512
NZ = 64
MEMBERS = 8
MODES = 256
REACH = 64


def draw_modes(key, part):
    first_key, second_key, third_key = jax.random.split(jax.random.fold_in(key, 7), 3)
    first = jax.random.randint(first_key, (MODES,), 0, NX // 2)
    second = jax.random.randint(second_key, (MODES,), 0, NY)
    third = jax.random.randint(third_key, (MODES,), 0, NZ)
    return jnp.stack([first, second, third]).astype(jnp.int32)


def steps_of(rng, shape, pieces, least, largest):
    loudness = 1.0
    for dim, parts in pieces:
        heights = jax.random.uniform(jax.random.fold_in(jax.random.fold_in(rng, 6), dim), (parts,), jnp.float32, least / len(pieces), largest / len(pieces))
        loudness = loudness * jnp.repeat(jnp.exp(heights), shape[dim] // parts).reshape((-1,) + (1,) * (len(shape) - 1 - dim))
    return loudness


def bell_draw(rng, extent, scale, reach, cuts=(), kind=jnp.bfloat16):
    entries = jax.random.normal(rng, extent, jnp.float32) * scale
    if len(cuts) > 0:
        entries = steps_of(rng, extent, cuts, -0.22, 0.18) * entries
    return jnp.clip(entries, min=-reach, max=reach).astype(kind)


def setup_inputs(seed: int = 0) -> dict:
    streams_of = jax.random.split(jax.random.key(seed), 3)
    return {
        "field": bell_draw(streams_of[0], (NY, NZ, MEMBERS, NX), 1.0, 6.0, ((0, 16), (1, 16)), jnp.float32),
        "modes": draw_modes(jax.random.fold_in(streams_of[2], 71), 0),
    }


def taper_of(modes):
    first = modes[0].astype(jnp.float32)
    second = jnp.where(modes[1] < NY // 2, modes[1], modes[1] - NY).astype(jnp.float32)
    third = jnp.where(modes[2] < NZ // 2, modes[2], modes[2] - NZ).astype(jnp.float32)
    first = jnp.concatenate([first, first])
    second = jnp.concatenate([second, second])
    third = jnp.concatenate([third, third])
    dist = (first[:, None] - first[None, :]) ** 2 + (second[:, None] - second[None, :]) ** 2
    dist = dist + (third[:, None] - third[None, :]) ** 2
    return jnp.exp(-dist / (2.0 * REACH * REACH))

def covariance_of(coef, modes):
    anomaly = coef - lax.optimization_barrier(jnp.mean(coef, axis=0, keepdims=True))
    cov = jnp.dot(anomaly.T, anomaly, precision=lax.Precision.HIGHEST) / (MEMBERS - 1)
    return cov * taper_of(modes)

def reference(field, modes):
    factor = 1.0 / math.sqrt(NX * NY * NZ)

    def one_member(member):
        whole = jnp.fft.fftn(member)[:, :, :NX // 2] * factor
        whole = jnp.transpose(whole, (1, 0, 2))
        paired = jnp.stack([jnp.real(whole), jnp.imag(whole)], axis=-1)
        return paired.reshape(NZ, NY, NX).astype(jnp.float32)
    stacked = lax.map(one_member, jnp.transpose(field, (2, 0, 1, 3)))
    spectrum = jnp.transpose(stacked, (1, 2, 0, 3))
    real_rows = spectrum[modes[2], modes[1], :, 2 * modes[0]]
    imag_rows = spectrum[modes[2], modes[1], :, 2 * modes[0] + 1]
    coef = jnp.concatenate([real_rows.T, imag_rows.T], axis=1)
    return (spectrum, covariance_of(coef, modes))
```

```python
import functools
import math

import jax
import jax.numpy as jnp
import numpy as np
from jax import lax
from jax.experimental import pallas as pl
from jax.experimental.pallas import tpu as pltpu
from jax.sharding import PartitionSpec as P

NX, NY, NZ, MEMBERS, MODES, REACH = 512, 512, 64, 8, 256, 64
PEERS = 16
LEVELS = NZ // PEERS
ROWS = NY // PEERS
CHUNKS = 8
AHEAD = 3
F32, BF16 = jnp.float32, jnp.bfloat16
MESH = pl.DeviceIdType.MESH
NT = (((1,), (1,)), ((), ()))
NN = (((1,), (0,)), ((), ()))


def halves(table):
    high = table.astype(jnp.bfloat16)
    low = (table - high.astype(np.float32)).astype(jnp.bfloat16)
    return np.stack([high, low])


@functools.cache
def x_table():
    half, block, part, wave = np.meshgrid(np.arange(2), np.arange(16), np.arange(2), np.arange(8), indexing="ij")
    kx = (block * 16 + half * 8 + wave).reshape(-1)
    part = part.reshape(-1)
    angle = 2 * np.pi * (kx[:, None] * np.arange(NX)[None, :] % NX) / NX
    table = np.where(part[:, None] == 0, np.cos(angle), -np.sin(angle)) / math.sqrt(NX * NY * NZ)
    return halves(table.astype(np.float32))


@functools.cache
def y_table():
    peer, out_part, low, out_member = np.meshgrid(np.arange(16), np.arange(2), np.arange(2), np.arange(8), indexing="ij")
    k2 = (peer * 2 + low).reshape(-1)[:, None]
    out_part, out_member = out_part.reshape(-1)[:, None], out_member.reshape(-1)[:, None]
    part, cell, member = np.meshgrid(np.arange(2), np.arange(32), np.arange(8), indexing="ij")
    part, cell, member = (a.reshape(-1)[None, :] for a in (part, cell, member))
    angle = 2 * np.pi * (cell * k2 % 32) / 32
    same = np.cos(angle)
    cross = np.where(out_part == 0, np.sin(angle), -np.sin(angle))
    table = np.where(out_part == part, same, cross) * (member == out_member)
    return halves(table.astype(np.float32))


@functools.cache
def y_twiddle():
    k1 = np.arange(16)[:, None]
    cell = (np.arange(256) // 8)[None, :]
    angle = 2 * np.pi * k1 * cell / NY
    return np.stack([np.cos(angle), np.sin(angle)], axis=1).reshape(32, 256).astype(np.float32)


@functools.cache
def lane_order():
    half, part, k1, wave = np.meshgrid(np.arange(2), np.arange(2), np.arange(16), np.arange(8), indexing="ij")
    target = (k1 * 32 + half * 16 + wave * 2 + part).reshape(-1)
    return (target[:, None] == np.arange(512)[None, :]).astype(jnp.bfloat16)


@functools.cache
def spread():
    part, cell, _ = np.meshgrid(np.arange(2), np.arange(32), np.arange(8), indexing="ij")
    source = (part * 32 + cell).reshape(-1)
    return (np.arange(128)[:, None] == source[None, :]).astype(jnp.bfloat16)


def quarter(a, b, c, d):
    (ar, ai), (br, bi), (cr, ci), (dr, di) = a, b, c, d
    s0r, s0i, s1r, s1i = ar + cr, ai + ci, ar - cr, ai - ci
    s2r, s2i, s3r, s3i = br + dr, bi + di, br - dr, bi - di
    return (
        (s0r + s2r, s0i + s2i),
        (s1r + s3i, s1i - s3r),
        (s0r - s2r, s0i - s2i),
        (s1r - s3i, s1i + s3r),
    )


def turn(value, numerator, denominator):
    re, im = value
    step = numerator % denominator
    if step == 0:
        return value
    if 4 * step == denominator:
        return (im, -re)
    if 8 * step == denominator:
        root = math.sqrt(0.5)
        return ((re + im) * root, (im - re) * root)
    if 8 * step == 3 * denominator:
        root = math.sqrt(0.5)
        return ((im - re) * root, -(re + im) * root)
    c = math.cos(2 * math.pi * step / denominator)
    s = math.sin(2 * math.pi * step / denominator)
    return (re * c + im * s, im * c - re * s)


def transform16(values):
    inner = [quarter(values[n], values[4 + n], values[8 + n], values[12 + n]) for n in range(4)]
    out = [None] * 16
    for k1 in range(4):
        column = [turn(inner[n][k1], n * k1, 16) for n in range(4)]
        for k2, value in enumerate(quarter(*column)):
            out[k1 + 4 * k2] = value
    return out


def split(value):
    high = value.astype(BF16)
    return high, (value - high.astype(F32)).astype(BF16)


def dot(a, b, dims):
    return lax.dot_general(a, b, dims, preferred_element_type=F32)


def cosine_of_turns(steps, period):
    turns = steps * (1.0 / period)
    turns = turns - jnp.floor(turns)
    s = (0.25 - jnp.abs(turns - 0.5)) * (2.0 * math.pi)
    s2 = s * s
    poly = 1.0 / 6227020800.0
    for c in (-1.0 / 39916800.0, 1.0 / 362880.0, -1.0 / 5040.0, 1.0 / 120.0, -1.0 / 6.0, 1.0):
        poly = poly * s2 + c
    return -(poly * s)


def exchange_kernel(
    field, modes, x_tab, y_tab, y_twid, spread_tab,
    levels_out, local_out,
    cells, x_t, y_t, tw, spr, cells_parts, lines, blocks, y_parts, waves,
    coef_one, coef_mine, coef_col, coef_row, coef_sum, coef_all, local_buf,
    load_sem, table_sem, row_send, row_recv, col_send, col_recv, own_sem,
    small_send, small_recv, local_sem,
):
    row, col = lax.axis_index("row"), lax.axis_index("col")
    z_at, y_lo = lax.rem(row, 8), row // 8

    def row_peer(k):
        return lax.rem(z_at + k, 8) + 8 * lax.rem(y_lo + k // 8, 2)

    def col_peer(k):
        return lax.rem(col + k, PEERS)

    barrier = pltpu.get_barrier_semaphore()

    @pl.loop(1, PEERS)
    def _(k):
        pl.semaphore_signal(barrier, inc=1, device_id={"row": row_peer(k)}, device_id_type=MESH)
        pl.semaphore_signal(barrier, inc=1, device_id={"col": col_peer(k)}, device_id_type=MESH)

    def load(level):
        return pltpu.make_async_copy(field.at[:, level], cells.at[level], load_sem.at[level])

    tables = [
        pltpu.make_async_copy(source, target, table_sem.at[i])
        for i, (source, target) in enumerate(((x_tab, x_t), (y_tab, y_t), (y_twid, tw), (spread_tab, spr)))
    ]
    tables[0].start()
    for level in range(LEVELS):
        load(level).start()
    for table in tables[1:]:
        table.start()

    def row_copy(chunk, k):
        peer = row_peer(k)
        return pltpu.make_async_remote_copy(
            src_ref=lines.at[chunk, peer], dst_ref=blocks.at[chunk, row],
            send_sem=row_send.at[chunk], recv_sem=row_recv.at[chunk],
            device_id={"row": peer}, device_id_type=MESH,
        )

    def col_copy(chunk, k):
        peer = col_peer(k)
        return pltpu.make_async_remote_copy(
            src_ref=waves.at[chunk, peer], dst_ref=levels_out.at[chunk, col],
            send_sem=col_send.at[chunk], recv_sem=col_recv.at[chunk],
            device_id={"col": peer}, device_id_type=MESH,
        )

    def own_copy(chunk):
        return pltpu.make_async_copy(waves.at[chunk, col], levels_out.at[chunk, col], own_sem.at[chunk])

    def wait_bytes(ref, sem):
        pltpu.make_async_copy(ref, ref, sem).wait()

    def send_rows(chunk):
        @pl.loop(1, PEERS)
        def _(k):
            row_copy(chunk, k).start()

    def x_transform(level, half):
        chunk = level * 2 + half
        table = pl.ds(half * 256, 256)
        high, low = cells_parts[0], cells_parts[1]
        value = dot(x_t[0, table], high, NT) + dot(x_t[0, table], low, NT) + dot(x_t[1, table], high, NT)
        lines[chunk] = value.reshape(PEERS, 16, 256)
        blocks[chunk, row] = lines[chunk, row]

    tables[0].wait()
    for level in range(LEVELS):
        load(level).wait()
        high, low = split(cells[level].reshape(256, NX))
        cells_parts[0], cells_parts[1] = high, low
        for half in range(2):
            x_transform(level, half)
            if level == 0 and half == 0:
                pl.semaphore_wait(barrier, 2 * (PEERS - 1))
            if level * 2 + half < AHEAD:
                send_rows(level * 2 + half)
    for table in tables[1:]:
        table.wait()

    def mode_row(i):
        return modes[i : i + 1, :].astype(F32)

    def down(value):
        return jnp.broadcast_to(value, (128, MODES)).T

    kx = mode_row(0)
    block = jnp.floor(kx * (1.0 / 16.0))
    half = jnp.floor((kx - 16.0 * block) * 0.125)
    place = half * 256.0 + block * 16.0 + (kx - 16.0 * block - 8.0 * half)
    place = down(place)
    lane = lax.broadcasted_iota(jnp.int32, (MODES, 128), 1)
    lane_f = lane.astype(F32)
    choose = jnp.concatenate(
        [
            jnp.concatenate([(place + 8.0 * part == lane_f + 128.0 * t).astype(F32) for t in range(4)], axis=1)
            for part in range(2)
        ],
        axis=0,
    ).astype(BF16)
    cell = lax.rem(lane, 32).astype(F32) + (row * ROWS).astype(F32)
    steps = down(mode_row(1)) * cell - jnp.where(lane >= 32, 128.0, 0.0)
    phase_high, phase_low = split(cosine_of_turns(steps, float(NY)))
    phase = dot(phase_high, spr[...], NN) + dot(phase_low, spr[...], NN)
    cos_y, sin_y = phase[:, :256], phase[:, 256:]
    level_row = lax.broadcasted_iota(jnp.int32, (8, MODES), 0)
    z_cell = lax.rem(level_row, 4).astype(F32) + (col * LEVELS).astype(F32)
    z_steps = mode_row(2) * z_cell - jnp.where(level_row >= 4, 16.0, 0.0)
    z_phase = cosine_of_turns(z_steps, float(NZ))
    gather_member = (
        lax.rem(lax.broadcasted_iota(jnp.int32, (8, 256), 1), 8) == lax.broadcasted_iota(jnp.int32, (8, 256), 0)
    ).astype(F32).astype(BF16)
    coef_re = jnp.zeros((8, MODES), F32)
    coef_im = jnp.zeros((8, MODES), F32)
    for level in range(LEVELS):
        high, low = split(lines[2 * level : 2 * level + 2].reshape(512, 256))
        at_modes = dot(choose, high, NN) + dot(choose, low, NN)
        re, im = at_modes[:MODES], at_modes[MODES:]
        out_re = re * cos_y + im * sin_y
        out_im = im * cos_y - re * sin_y
        sums = []
        for value in (out_re, out_im):
            high, low = split(value)
            sums.append(dot(gather_member, high, NT) + dot(gather_member, low, NT))
        c, s = z_phase[level : level + 1], z_phase[4 + level : 5 + level]
        coef_re += sums[0] * c + sums[1] * s
        coef_im += sums[1] * c - sums[0] * s
    for t in range(2):
        coef_one[t] = coef_re[:, 128 * t : 128 * t + 128]
        coef_one[2 + t] = coef_im[:, 128 * t : 128 * t + 128]

    def tile_copy(k):
        peer = col_peer(k)
        return pltpu.make_async_remote_copy(
            src_ref=coef_one.at[lax.rem(peer, 4)], dst_ref=coef_col.at[col],
            send_sem=small_send.at[0], recv_sem=small_recv.at[0], device_id={"col": peer}, device_id_type=MESH,
        )

    def sum_copy(k):
        return pltpu.make_async_remote_copy(
            src_ref=coef_mine, dst_ref=coef_row.at[row],
            send_sem=small_send.at[1], recv_sem=small_recv.at[1], device_id={"row": row_peer(k)}, device_id_type=MESH,
        )

    def share_copy(k):
        peer = (col // 4) * 4 + lax.rem(col + k, 4)
        return pltpu.make_async_remote_copy(
            src_ref=coef_sum, dst_ref=coef_all.at[lax.rem(col, 4)],
            send_sem=small_send.at[2], recv_sem=small_recv.at[2], device_id={"col": peer}, device_id_type=MESH,
        )

    def start_all(copy, count):
        @pl.loop(1, count)
        def _(k):
            copy(k).start()

    coef_col[col] = coef_one[lax.rem(col, 4)]
    start_all(tile_copy, PEERS)

    def small_step(step):
        if step == 0:
            wait_bytes(coef_col.at[pl.ds(0, PEERS - 1)], small_recv.at[0])
            total = coef_col[0]
            for i in range(1, PEERS):
                total = total + coef_col[i]
            coef_mine[...] = total
            coef_row[row] = total
            start_all(sum_copy, PEERS)
        elif step == 1:
            wait_bytes(coef_row.at[pl.ds(0, PEERS - 1)], small_recv.at[1])
            total = coef_row[0]
            for i in range(1, PEERS):
                total = total + coef_row[i]
            coef_sum[...] = total
            coef_all[lax.rem(col, 4)] = total
            start_all(share_copy, 4)
        else:
            wait_bytes(coef_all.at[pl.ds(0, 3)], small_recv.at[2])
            coef = jnp.concatenate([coef_all[i] for i in range(4)], axis=1)
            anomaly = coef - jnp.mean(coef, axis=0, keepdims=True)
            turned = anomaly.T
            a_high, a_low = split(turned)
            b_high, b_low = split(anomaly)
            kx, ky, kz = mode_row(0), mode_row(1), mode_row(2)
            ky = jnp.where(ky < NY // 2, ky, ky - NY)
            kz = jnp.where(kz < NZ // 2, kz, kz - NZ)
            dist = jnp.zeros((MODES, MODES), F32)
            for wave in (kx, ky, kz):
                tall = down(wave)
                tall = jnp.concatenate([tall, tall], axis=1)
                dist += (tall - wave) ** 2
            taper = jnp.exp(-dist * (1.0 / (2.0 * REACH * REACH))) * (1.0 / (MEMBERS - 1))
            for i in range(2):
                at = slice(i * MODES, (i + 1) * MODES)
                cov = dot(a_high[at], b_high, NN) + dot(a_high[at], b_low, NN) + dot(a_low[at], b_high, NN)
                local_buf[at, :MODES] = cov[:, :MODES] * taper
                local_buf[at, MODES:] = cov[:, MODES:] * taper
            pltpu.make_async_copy(local_buf, local_out, local_sem).start()

    @pl.loop(0, CHUNKS)
    def _(chunk):
        @pl.when(chunk + AHEAD < CHUNKS)
        def _():
            send_rows(chunk + AHEAD)

        wait_bytes(blocks.at[chunk, pl.ds(0, PEERS - 1)], row_recv.at[chunk])
        for t in range(2):
            lanes = pl.ds(t * 128, 128)
            values = [(blocks[chunk, i, 0:8, lanes], blocks[chunk, i, 8:16, lanes]) for i in range(16)]
            out = transform16(values)
            for pair in range(8):
                parts = []
                for k1 in (2 * pair, 2 * pair + 1):
                    re, im = out[k1]
                    if k1 > 0:
                        c = tw[2 * k1 : 2 * k1 + 1, lanes]
                        s = tw[2 * k1 + 1 : 2 * k1 + 2, lanes]
                        re, im = re * c + im * s, im * c - re * s
                    parts.append((re, im))
                for part in range(2):
                    value = jnp.concatenate([parts[0][part], parts[1][part]], axis=0)
                    high, low = split(value)
                    at = pl.ds(part * 256 + t * 128, 128)
                    y_parts[pl.ds(16 * pair, 16), at] = high
                    y_parts[pl.ds(128 + 16 * pair, 16), at] = low
        both = dot(y_t[0], y_parts[...], NT)
        value = both[:, :128] + both[:, 128:] + dot(y_t[1], y_parts[pl.ds(0, 128)], NT)
        waves[chunk] = value.reshape(PEERS, 32, 128)

        @pl.loop(1, PEERS)
        def _(k):
            col_copy(chunk, k).start()

        own_copy(chunk).start()

        for step, at in enumerate((1, 3, 5)):
            @pl.when(chunk == at)
            def _(step=step):
                small_step(step)

    pltpu.make_async_copy(local_buf, local_out, local_sem).wait()
    wait_bytes(coef_col.at[pl.ds(0, PEERS - 1)], small_send.at[0])
    wait_bytes(coef_row.at[pl.ds(0, PEERS - 1)], small_send.at[1])
    wait_bytes(coef_all.at[pl.ds(0, 3)], small_send.at[2])

    @pl.loop(0, CHUNKS)
    def _(chunk):
        wait_bytes(lines.at[chunk, pl.ds(0, PEERS - 1)], row_send.at[chunk])
        wait_bytes(waves.at[chunk, pl.ds(0, PEERS - 1)], col_send.at[chunk])
        own_copy(chunk).wait()
        wait_bytes(levels_out.at[chunk, pl.ds(0, PEERS - 1)], col_recv.at[chunk])


def exchange(field, modes):
    any_space = pl.BlockSpec(memory_space=pl.ANY)
    dma = pltpu.SemaphoreType.DMA
    return pl.pallas_call(
        exchange_kernel,
        out_shape=(
            jax.ShapeDtypeStruct((CHUNKS, PEERS, 32, 128), F32),
            jax.ShapeDtypeStruct((2 * MODES, 2 * MODES), F32),
        ),
        in_specs=[any_space, pl.BlockSpec(memory_space=pltpu.VMEM)] + [any_space] * 4,
        out_specs=(any_space, any_space),
        scratch_shapes=[
            pltpu.VMEM((LEVELS, ROWS, MEMBERS, NX), F32),
            pltpu.VMEM((2, 512, 512), BF16),
            pltpu.VMEM((2, 512, 512), BF16),
            pltpu.VMEM((32, 256), F32),
            pltpu.VMEM((128, 512), BF16),
            pltpu.VMEM((2, 256, NX), BF16),
            pltpu.VMEM((CHUNKS, PEERS, 16, 256), F32),
            pltpu.VMEM((CHUNKS, PEERS, 16, 256), F32),
            pltpu.VMEM((256, 512), BF16),
            pltpu.VMEM((CHUNKS, PEERS, 32, 128), F32),
            pltpu.VMEM((4, 8, 128), F32),
            pltpu.VMEM((8, 128), F32),
            pltpu.VMEM((PEERS, 8, 128), F32),
            pltpu.VMEM((PEERS, 8, 128), F32),
            pltpu.VMEM((8, 128), F32),
            pltpu.VMEM((4, 8, 128), F32),
            pltpu.VMEM((512, 512), F32),
            dma((LEVELS,)),
            dma((4,)),
            dma((CHUNKS,)),
            dma((CHUNKS,)),
            dma((CHUNKS,)),
            dma((CHUNKS,)),
            dma((CHUNKS,)),
            dma((3,)),
            dma((3,)),
            dma,
        ],
        compiler_params=pltpu.CompilerParams(collective_id=0, has_side_effects=True, vmem_limit_bytes=48 << 20),
        cost_estimate=pl.CostEstimate(flops=10**10, bytes_accessed=8 << 20, transcendentals=0),
        name="exchange",
    )(field, modes, x_table(), y_table(), y_twiddle(), spread())


def levels_kernel(levels, order, local_in, spectrum, local, inner, rows):
    group = pl.program_id(1)

    @pl.when(group == 0)
    def _():
        for level in range(LEVELS):
            for half in range(2):
                values = [
                    (levels[2 * level + half, i, 0, 0], levels[2 * level + half, i, 1, 0]) for i in range(PEERS)
                ]
                for a, value in enumerate(transform16(values)):
                    value = turn(value, level * a, NZ)
                    for part in range(2):
                        inner[half, part, level, a] = value[part]

    for i in range(4):
        a = group * 4 + i
        for half in range(2):
            values = [(inner[half, 0, n, a], inner[half, 1, n, a]) for n in range(LEVELS)]
            for b, value in enumerate(quarter(*values)):
                for part in range(2):
                    at = pl.ds((half * 2 + part) * 128, 128)
                    rows[pl.ds((b * 4 + i) * 8, 8), at] = value[part]
    high, low = split(rows[...])
    value = dot(high, order[...], NN) + dot(low, order[...], NN)
    for b in range(4):
        for i in range(4):
            for k1 in range(16):
                at = (b * 4 + i) * 8
                spectrum[b, i, k1] = value[at : at + 8, 32 * k1 : 32 * k1 + 32]
    local[...] = local_in[...]


def from_levels(levels, local):
    levels = levels.reshape(CHUNKS, PEERS, 2, 2, 8, 128)
    block = 2 * MODES // 8
    spectrum, local = pl.pallas_call(
        levels_kernel,
        grid=(2, 4),
        out_shape=(
            jax.ShapeDtypeStruct((4, 16, 32, 8, 32), F32),
            jax.ShapeDtypeStruct((2 * MODES, 2 * MODES), F32),
        ),
        in_specs=[
            pl.BlockSpec((CHUNKS, PEERS, 2, 1, 8, 128), lambda low, group: (0, 0, 0, low, 0, 0)),
            pl.BlockSpec((512, 512), lambda low, group: (0, 0)),
            pl.BlockSpec((block, 2 * MODES), lambda low, group: (low * 4 + group, 0)),
        ],
        out_specs=(
            pl.BlockSpec((4, 4, 16, 8, 32), lambda low, group: (0, group, low, 0, 0)),
            pl.BlockSpec((block, 2 * MODES), lambda low, group: (low * 4 + group, 0)),
        ),
        scratch_shapes=[
            pltpu.VMEM((2, 2, LEVELS, 16, 8, 128), F32),
            pltpu.VMEM((128, 512), F32),
        ],
        compiler_params=pltpu.CompilerParams(vmem_limit_bytes=32 << 20),
        cost_estimate=pl.CostEstimate(flops=10**9, bytes_accessed=10 << 20, transcendentals=0),
        name="from_levels",
    )(levels, lane_order(), local)
    return spectrum.reshape(NZ, NY // PEERS, MEMBERS, 2 * NX // 32), local


def per_device(field, modes):
    levels, local = exchange(field, modes)
    return from_levels(levels, local)


def solution(mesh):
    return jax.shard_map(
        per_device,
        mesh=mesh,
        in_specs=(P("row", "col", None, None), P()),
        out_specs=(P(None, "col", None, "row"), P()),
        check_vma=False,
    )
```

```python
import functools
import math

import jax
import jax.numpy as jnp
import numpy as np
from jax import lax
from jax.experimental import pallas as pl
from jax.experimental.pallas import tpu as pltpu
from jax.sharding import PartitionSpec as P

NX, NY, NZ, MEMBERS, MODES, REACH = 512, 512, 64, 8, 256, 64
PEERS = 16
LEVELS = NZ // PEERS
ROWS = NY // PEERS
PAIRS = 4
CHUNKS = 8
AHEAD = 3
VMEM = 67_043_328
F32, BF16 = jnp.float32, jnp.bfloat16
MESH = pl.DeviceIdType.MESH
NT = (((1,), (1,)), ((), ()))
NN = (((1,), (0,)), ((), ()))


def halves(table):
    high = table.astype(jnp.bfloat16)
    low = (table - high.astype(np.float32)).astype(jnp.bfloat16)
    return np.stack([high, low])


@functools.cache
def x_table():
    half, block, part, wave = np.meshgrid(np.arange(2), np.arange(16), np.arange(2), np.arange(8), indexing="ij")
    kx = (block * 16 + half * 8 + wave).reshape(-1)
    part = part.reshape(-1)
    angle = 2 * np.pi * (kx[:, None] * np.arange(NX)[None, :] % NX) / NX
    table = np.where(part[:, None] == 0, np.cos(angle), -np.sin(angle)) / math.sqrt(NX * NY * NZ)
    return halves(table.astype(np.float32))


@functools.cache
def y_table():
    rows = np.meshgrid(np.arange(16), np.arange(2), np.arange(2), np.arange(2), np.arange(4), indexing="ij")
    peer, out_part, low, out_member, out_level = (a.reshape(-1)[:, None] for a in rows)
    columns = np.meshgrid(np.arange(2), np.arange(2), np.arange(32), np.arange(4), indexing="ij")
    part, member, cell, level = (a.reshape(-1)[None, :] for a in columns)
    angle = 2 * np.pi * (cell * (peer * 2 + low) % 32) / 32
    cross = np.where(out_part == 0, np.sin(angle), -np.sin(angle))
    table = np.where(out_part == part, np.cos(angle), cross) * (member == out_member) * (level == out_level)
    return halves(table.astype(np.float32))


@functools.cache
def y_twiddle():
    k1 = np.arange(16)[:, None]
    cell = (np.arange(128) // 4)[None, :]
    angle = 2 * np.pi * k1 * cell / NY
    return np.stack([np.cos(angle), np.sin(angle)], axis=1).reshape(32, 128).astype(np.float32)


@functools.cache
def z_table():
    rows = np.meshgrid(np.arange(16), np.arange(2), np.arange(2), np.arange(4), indexing="ij")
    peer, part, member, level = (a.reshape(-1)[:, None] for a in rows)
    columns = np.meshgrid(np.arange(2), np.arange(2), np.arange(64), indexing="ij")
    out_part, out_member, kz = (a.reshape(-1)[None, :] for a in columns)
    angle = 2 * np.pi * ((4 * peer + level) * kz % NZ) / NZ
    cross = np.where(out_part == 0, np.sin(angle), -np.sin(angle))
    table = np.where(out_part == part, np.cos(angle), cross) * (member == out_member)
    return halves(table.astype(np.float32))


def quarter(a, b, c, d):
    (ar, ai), (br, bi), (cr, ci), (dr, di) = a, b, c, d
    s0r, s0i, s1r, s1i = ar + cr, ai + ci, ar - cr, ai - ci
    s2r, s2i, s3r, s3i = br + dr, bi + di, br - dr, bi - di
    return (
        (s0r + s2r, s0i + s2i),
        (s1r + s3i, s1i - s3r),
        (s0r - s2r, s0i - s2i),
        (s1r - s3i, s1i + s3r),
    )


def turn(value, numerator, denominator):
    re, im = value
    step = numerator % denominator
    if step == 0:
        return value
    if 4 * step == denominator:
        return (im, -re)
    if 8 * step == denominator:
        root = math.sqrt(0.5)
        return ((re + im) * root, (im - re) * root)
    if 8 * step == 3 * denominator:
        root = math.sqrt(0.5)
        return ((im - re) * root, -(re + im) * root)
    c = math.cos(2 * math.pi * step / denominator)
    s = math.sin(2 * math.pi * step / denominator)
    return (re * c + im * s, im * c - re * s)


def transform16(values):
    inner = [quarter(values[n], values[4 + n], values[8 + n], values[12 + n]) for n in range(4)]
    out = [None] * 16
    for k1 in range(4):
        column = [turn(inner[n][k1], n * k1, 16) for n in range(4)]
        for k2, value in enumerate(quarter(*column)):
            out[k1 + 4 * k2] = value
    return out


def split(value):
    high = value.astype(BF16)
    return high, (value - high.astype(F32)).astype(BF16)


def dot(a, b, dims):
    return lax.dot_general(a, b, dims, preferred_element_type=F32)


def cosine_of_turns(steps, period):
    turns = steps * (1.0 / period)
    turns = turns - jnp.floor(turns)
    s = (0.25 - jnp.abs(turns - 0.5)) * (2.0 * math.pi)
    s2 = s * s
    poly = 1.0 / 6227020800.0
    for c in (-1.0 / 39916800.0, 1.0 / 362880.0, -1.0 / 5040.0, 1.0 / 120.0, -1.0 / 6.0, 1.0):
        poly = poly * s2 + c
    return -(poly * s)


def exchange_kernel(
    field, modes_in, x_tab, y_tab, y_twid,
    levels_out, local_out,
    cells, modes, x_t, y_t, tw, cells_parts, lines, blocks, y_parts, waves,
    coef_one, coef_mine, coef_col, coef_row, coef_sum, coef_all, local_buf,
    load_sem, row_send, row_recv, col_send, col_recv, own_sem,
    small_send, small_recv, local_sem,
):
    row, col = lax.axis_index("row"), lax.axis_index("col")
    z_at, y_lo = lax.rem(row, 8), row // 8

    def row_peer(k):
        return lax.rem(z_at + k, 8) + 8 * lax.rem(y_lo + k // 8, 2)

    def col_peer(k):
        return lax.rem(col + k, PEERS)

    barrier = pltpu.get_barrier_semaphore()

    @pl.loop(1, PEERS)
    def _(k):
        pl.semaphore_signal(barrier, inc=1, device_id={"row": row_peer(k)}, device_id_type=MESH)
        pl.semaphore_signal(barrier, inc=1, device_id={"col": col_peer(k)}, device_id_type=MESH)

    pieces = [(x_tab, x_t)] + [(field.at[:, pl.ds(128 * t, 128)], cells.at[t]) for t in range(NX // 128)]
    first_pieces = len(pieces)
    pieces += [(modes_in, modes), (y_twid, tw), (y_tab, y_t)]
    loads = [pltpu.make_async_copy(source, target, load_sem.at[i]) for i, (source, target) in enumerate(pieces)]
    for each in loads:
        each.start()

    def row_copy(chunk, k):
        peer = row_peer(k)
        return pltpu.make_async_remote_copy(
            src_ref=lines.at[chunk, peer], dst_ref=blocks.at[chunk, row],
            send_sem=row_send.at[chunk], recv_sem=row_recv.at[chunk],
            device_id={"row": peer}, device_id_type=MESH,
        )

    def col_copy(chunk, k):
        peer = col_peer(k)
        return pltpu.make_async_remote_copy(
            src_ref=waves.at[chunk, peer], dst_ref=levels_out.at[chunk, col],
            send_sem=col_send.at[chunk], recv_sem=col_recv.at[chunk],
            device_id={"col": peer}, device_id_type=MESH,
        )

    def own_copy(chunk):
        return pltpu.make_async_copy(waves.at[chunk, col], levels_out.at[chunk, col], own_sem.at[chunk])

    def wait_bytes(ref, sem):
        pltpu.make_async_copy(ref, ref, sem).wait()

    def send_rows(chunk):
        @pl.loop(1, PEERS)
        def _(k):
            row_copy(chunk, k).start()

    for each in loads[:first_pieces]:
        each.wait()
    for pair in range(PAIRS):
        for i in range(2):
            for t in range(NX // 128):
                high, low = split(cells[t, pl.ds(2 * pair + i, ROWS * LEVELS, stride=MEMBERS), :])
                at = (pl.ds(i * 128, 128), pl.ds(t * 128, 128))
                cells_parts[(0, *at)], cells_parts[(1, *at)] = high, low
        for half in range(2):
            chunk = pair * 2 + half
            table = pl.ds(half * 256, 256)
            high, low = cells_parts[0], cells_parts[1]
            value = dot(x_t[0, table], high, NT) + dot(x_t[0, table], low, NT) + dot(x_t[1, table], high, NT)
            lines[chunk] = value.reshape(PEERS, 16, 256)
            blocks[chunk, row] = lines[chunk, row]
            if chunk == 0:
                pl.semaphore_wait(barrier, 2 * (PEERS - 1))
            if chunk < AHEAD:
                send_rows(chunk)
    for each in loads[first_pieces:]:
        each.wait()

    def mode_row(i):
        return modes[i : i + 1, :].astype(F32)

    def down(value):
        return jnp.broadcast_to(value, (128, MODES)).T

    kx = mode_row(0)
    block = jnp.floor(kx * (1.0 / 16.0))
    half = jnp.floor((kx - 16.0 * block) * 0.125)
    place = half * 256.0 + block * 16.0 + (kx - 16.0 * block - 8.0 * half)
    place = down(place)
    lane = lax.broadcasted_iota(jnp.int32, (MODES, 128), 1)
    lane_f = lane.astype(F32)
    choose = jnp.concatenate(
        [
            jnp.concatenate([(place + 8.0 * part == lane_f + 128.0 * t).astype(F32) for t in range(4)], axis=1)
            for part in range(2)
        ],
        axis=0,
    ).astype(BF16)
    cell = (lane // 4).astype(F32) + (row * ROWS).astype(F32)
    level = lax.rem(lane, 4).astype(F32) + (col * LEVELS).astype(F32)
    steps = down(mode_row(1)) * cell + down(mode_row(2)) * level * float(NY // NZ)
    cos = cosine_of_turns(steps, float(NY))
    sin = cosine_of_turns(steps - 128.0, float(NY))
    cos, sin = jnp.concatenate([cos, cos], axis=1), jnp.concatenate([sin, sin], axis=1)
    lane_member = lax.broadcasted_iota(jnp.int32, (8, 256), 1) // 128
    member = lax.broadcasted_iota(jnp.int32, (8, 256), 0)
    coef_re = jnp.zeros((8, MODES), F32)
    coef_im = jnp.zeros((8, MODES), F32)
    for pair in range(PAIRS):
        gather_member = (lane_member + 2 * pair == member).astype(F32).astype(BF16)
        high, low = split(lines[2 * pair : 2 * pair + 2].reshape(512, 256))
        at_modes = dot(choose, high, NN) + dot(choose, low, NN)
        re, im = at_modes[:MODES], at_modes[MODES:]
        sums = []
        for value in (re * cos + im * sin, im * cos - re * sin):
            high, low = split(value)
            sums.append(dot(gather_member, high, NT) + dot(gather_member, low, NT))
        coef_re += sums[0]
        coef_im += sums[1]
    for t in range(2):
        coef_one[t] = coef_re[:, 128 * t : 128 * t + 128]
        coef_one[2 + t] = coef_im[:, 128 * t : 128 * t + 128]

    def tile_copy(k):
        peer = col_peer(k)
        return pltpu.make_async_remote_copy(
            src_ref=coef_one.at[lax.rem(peer, 4)], dst_ref=coef_col.at[col],
            send_sem=small_send.at[0], recv_sem=small_recv.at[0], device_id={"col": peer}, device_id_type=MESH,
        )

    def sum_copy(k):
        return pltpu.make_async_remote_copy(
            src_ref=coef_mine, dst_ref=coef_row.at[row],
            send_sem=small_send.at[1], recv_sem=small_recv.at[1], device_id={"row": row_peer(k)}, device_id_type=MESH,
        )

    def share_copy(k):
        peer = (col // 4) * 4 + lax.rem(col + k, 4)
        return pltpu.make_async_remote_copy(
            src_ref=coef_sum, dst_ref=coef_all.at[lax.rem(col, 4)],
            send_sem=small_send.at[2], recv_sem=small_recv.at[2], device_id={"col": peer}, device_id_type=MESH,
        )

    def start_all(copy, count):
        @pl.loop(1, count)
        def _(k):
            copy(k).start()

    coef_col[col] = coef_one[lax.rem(col, 4)]
    start_all(tile_copy, PEERS)

    def small_step(step):
        if step == 0:
            wait_bytes(coef_col.at[pl.ds(0, PEERS - 1)], small_recv.at[0])
            total = coef_col[0]
            for i in range(1, PEERS):
                total = total + coef_col[i]
            coef_mine[...] = total
            coef_row[row] = total
            start_all(sum_copy, PEERS)
        elif step == 1:
            wait_bytes(coef_row.at[pl.ds(0, PEERS - 1)], small_recv.at[1])
            total = coef_row[0]
            for i in range(1, PEERS):
                total = total + coef_row[i]
            coef_sum[...] = total
            coef_all[lax.rem(col, 4)] = total
            start_all(share_copy, 4)
        else:
            wait_bytes(coef_all.at[pl.ds(0, 3)], small_recv.at[2])
            coef = jnp.concatenate([coef_all[i] for i in range(4)], axis=1)
            anomaly = coef - jnp.mean(coef, axis=0, keepdims=True)
            turned = anomaly.T
            a_high, a_low = split(turned)
            b_high, b_low = split(anomaly)
            kx, ky, kz = mode_row(0), mode_row(1), mode_row(2)
            ky = jnp.where(ky < NY // 2, ky, ky - NY)
            kz = jnp.where(kz < NZ // 2, kz, kz - NZ)
            dist = jnp.zeros((MODES, MODES), F32)
            for wave in (kx, ky, kz):
                tall = down(wave)
                tall = jnp.concatenate([tall, tall], axis=1)
                dist += (tall - wave) ** 2
            taper = jnp.exp(-dist * (1.0 / (2.0 * REACH * REACH))) * (1.0 / (MEMBERS - 1))
            for i in range(2):
                at = slice(i * MODES, (i + 1) * MODES)
                cov = dot(a_high[at], b_high, NN) + dot(a_high[at], b_low, NN) + dot(a_low[at], b_high, NN)
                local_buf[at, :MODES] = cov[:, :MODES] * taper
                local_buf[at, MODES:] = cov[:, MODES:] * taper
            pltpu.make_async_copy(local_buf, local_out, local_sem).start()

    @pl.loop(0, CHUNKS)
    def _(chunk):
        @pl.when(chunk + AHEAD < CHUNKS)
        def _():
            send_rows(chunk + AHEAD)

        wait_bytes(blocks.at[chunk, pl.ds(0, PEERS - 1)], row_recv.at[chunk])
        for t in range(2):
            lanes = pl.ds(t * 128, 128)
            values = [(blocks[chunk, i, 0:8, lanes], blocks[chunk, i, 8:16, lanes]) for i in range(16)]
            out = transform16(values)
            for pair in range(8):
                parts = []
                for k1 in (2 * pair, 2 * pair + 1):
                    re, im = out[k1]
                    if k1 > 0:
                        c = tw[2 * k1 : 2 * k1 + 1, :]
                        s = tw[2 * k1 + 1 : 2 * k1 + 2, :]
                        re, im = re * c + im * s, im * c - re * s
                    parts.append((re, im))
                for part in range(2):
                    value = jnp.concatenate([parts[0][part], parts[1][part]], axis=0)
                    high, low = split(value)
                    at = pl.ds(part * 256 + t * 128, 128)
                    y_parts[pl.ds(16 * pair, 16), at] = high
                    y_parts[pl.ds(128 + 16 * pair, 16), at] = low
        both = dot(y_t[0], y_parts[...], NT)
        value = both[:, :128] + both[:, 128:] + dot(y_t[1], y_parts[pl.ds(0, 128)], NT)
        waves[chunk] = value.reshape(PEERS, 32, 128)

        @pl.loop(1, PEERS)
        def _(k):
            col_copy(chunk, k).start()

        own_copy(chunk).start()

        for step, at in enumerate((1, 3, 5)):
            @pl.when(chunk == at)
            def _(step=step):
                small_step(step)

    pltpu.make_async_copy(local_buf, local_out, local_sem).wait()
    wait_bytes(coef_col.at[pl.ds(0, PEERS - 1)], small_send.at[0])
    wait_bytes(coef_row.at[pl.ds(0, PEERS - 1)], small_send.at[1])
    wait_bytes(coef_all.at[pl.ds(0, 3)], small_send.at[2])

    @pl.loop(0, CHUNKS)
    def _(chunk):
        wait_bytes(lines.at[chunk, pl.ds(0, PEERS - 1)], row_send.at[chunk])
        wait_bytes(waves.at[chunk, pl.ds(0, PEERS - 1)], col_send.at[chunk])
        own_copy(chunk).wait()
        wait_bytes(levels_out.at[chunk, pl.ds(0, PEERS - 1)], col_recv.at[chunk])


def exchange(field, modes):
    any_space = pl.BlockSpec(memory_space=pl.ANY)
    dma = pltpu.SemaphoreType.DMA
    return pl.pallas_call(
        exchange_kernel,
        out_shape=(
            jax.ShapeDtypeStruct((CHUNKS, PEERS, 32, 128), F32),
            jax.ShapeDtypeStruct((2 * MODES, 2 * MODES), F32),
        ),
        in_specs=[any_space] * 5,
        out_specs=(any_space, any_space),
        scratch_shapes=[
            pltpu.VMEM((NX // 128, ROWS * LEVELS * MEMBERS, 128), F32),
            pltpu.VMEM((3, MODES), jnp.int32),
            pltpu.VMEM((2, 512, 512), BF16),
            pltpu.VMEM((2, 512, 512), BF16),
            pltpu.VMEM((32, 128), F32),
            pltpu.VMEM((2, 256, NX), BF16),
            pltpu.VMEM((CHUNKS, PEERS, 16, 256), F32),
            pltpu.VMEM((CHUNKS, PEERS, 16, 256), F32),
            pltpu.VMEM((256, 512), BF16),
            pltpu.VMEM((CHUNKS, PEERS, 32, 128), F32),
            pltpu.VMEM((4, 8, 128), F32),
            pltpu.VMEM((8, 128), F32),
            pltpu.VMEM((PEERS, 8, 128), F32),
            pltpu.VMEM((PEERS, 8, 128), F32),
            pltpu.VMEM((8, 128), F32),
            pltpu.VMEM((4, 8, 128), F32),
            pltpu.VMEM((512, 512), F32),
            dma((8,)),
            dma((CHUNKS,)),
            dma((CHUNKS,)),
            dma((CHUNKS,)),
            dma((CHUNKS,)),
            dma((CHUNKS,)),
            dma((3,)),
            dma((3,)),
            dma,
        ],
        compiler_params=pltpu.CompilerParams(collective_id=0, has_side_effects=True, vmem_limit_bytes=VMEM),
        cost_estimate=pl.CostEstimate(flops=10**10, bytes_accessed=8 << 20, transcendentals=0),
        name="exchange",
    )(field.reshape(-1, NX), modes, x_table(), y_table(), y_twiddle())


def levels_kernel(levels, table, local_in, spectrum, local, rows):
    for half in range(2):
        for low_k in range(2):
            value = levels[half, :, :, low_k].reshape(256, 128).T
            high, low = split(value)
            out = dot(high, table[0], NN) + dot(high, table[1], NN) + dot(low, table[0], NN)
            for k1 in range(16):
                for part in range(2):
                    at = (low_k * 16 + k1) * 32 + 16 * half + part
                    rows[pl.ds(at, 8, stride=2), :] = out[8 * k1 : 8 * k1 + 8, 128 * part : 128 * part + 128]
    value = rows[...].reshape(NY // PEERS, 32, 128)
    for member in range(2):
        spectrum[:, member] = value[:, :, member * NZ : (member + 1) * NZ]
    local[...] = local_in[...]


def from_levels(levels, local):
    levels = levels.reshape(CHUNKS, PEERS, 2, 2, 8, 128)
    block = 2 * MODES // PAIRS
    spectrum, local = pl.pallas_call(
        levels_kernel,
        grid=(PAIRS,),
        out_shape=(
            jax.ShapeDtypeStruct((NY // PEERS, MEMBERS, 32, NZ), F32),
            jax.ShapeDtypeStruct((2 * MODES, 2 * MODES), F32),
        ),
        in_specs=[
            pl.BlockSpec((2, PEERS, 2, 2, 8, 128), lambda pair: (pair, 0, 0, 0, 0, 0)),
            pl.BlockSpec((2, 256, 256), lambda pair: (0, 0, 0)),
            pl.BlockSpec((block, 2 * MODES), lambda pair: (pair, 0)),
        ],
        out_specs=(
            pl.BlockSpec((NY // PEERS, 2, 32, NZ), lambda pair: (0, pair, 0, 0)),
            pl.BlockSpec((block, 2 * MODES), lambda pair: (pair, 0)),
        ),
        scratch_shapes=[pltpu.VMEM((NY // PEERS * 32, 128), F32)],
        compiler_params=pltpu.CompilerParams(vmem_limit_bytes=VMEM),
        cost_estimate=pl.CostEstimate(flops=10**9, bytes_accessed=8 << 20, transcendentals=0),
        name="from_levels",
    )(levels, z_table(), local)
    return jnp.transpose(spectrum, (3, 0, 1, 2)), local


def per_device(field, modes):
    levels, local = exchange(field, modes)
    return from_levels(levels, local)


def solution(mesh):
    return jax.shard_map(
        per_device,
        mesh=mesh,
        in_specs=(P("row", "col", None, None), P()),
        out_specs=(P(None, "col", None, "row"), P()),
        check_vma=False,
    )
```

```python
import functools
import math

import jax
import jax.numpy as jnp
import numpy as np
from jax import lax
from jax.experimental import pallas as pl
from jax.experimental.pallas import tpu as pltpu
from jax.sharding import PartitionSpec as P

NX, NY, NZ, MEMBERS, MODES, REACH = 512, 512, 64, 8, 256, 64
PEERS = 16
LEVELS = NZ // PEERS
ROWS = NY // PEERS
CHUNKS = 2 * MEMBERS
AHEAD = 4
PLANES = (0, 1, 2, 3, 7, 6, 4, 5)
LEAD = (1, 0, 0, 0, 0, 0, 0, 0)
VMEM = 67_043_328 - (3 << 20) - (256 << 10)
F32, BF16 = jnp.float32, jnp.bfloat16
MESH = pl.DeviceIdType.MESH
NT = (((1,), (1,)), ((), ()))
NN = (((1,), (0,)), ((), ()))


def halves(table):
    high = table.astype(jnp.bfloat16)
    low = (table - high.astype(np.float32)).astype(jnp.bfloat16)
    return np.stack([high, low])


@functools.cache
def x_table():
    half, block, part, wave = np.meshgrid(np.arange(2), np.arange(16), np.arange(2), np.arange(8), indexing="ij")
    kx = (block * 16 + half * 8 + wave).reshape(-1)
    part = part.reshape(-1)
    angle = 2 * np.pi * (kx[:, None] * np.arange(NX)[None, :] % NX) / NX
    table = np.where(part[:, None] == 0, np.cos(angle), -np.sin(angle)) / math.sqrt(NX * NY * NZ)
    return halves(table.astype(np.float32))


@functools.cache
def y_table():
    rows = np.meshgrid(np.arange(16), np.arange(2), np.arange(2), np.arange(4), indexing="ij")
    peer, out_part, low, out_level = (a.reshape(-1)[:, None] for a in rows)
    columns = np.meshgrid(np.arange(2), np.arange(32), np.arange(4), indexing="ij")
    part, cell, level = (a.reshape(-1)[None, :] for a in columns)
    angle = 2 * np.pi * (cell * (peer * 2 + low) % 32) / 32
    cross = np.where(out_part == 0, np.sin(angle), -np.sin(angle))
    table = np.where(out_part == part, np.cos(angle), cross) * (level == out_level)
    return halves(table.astype(np.float32))


@functools.cache
def y_twiddle():
    k1 = np.arange(16)[:, None]
    cell = (np.arange(128) // 4)[None, :]
    angle = 2 * np.pi * k1 * cell / NY
    return np.stack([np.cos(angle), np.sin(angle)], axis=1).reshape(32, 128).astype(np.float32)


@functools.cache
def z_table():
    rows = np.meshgrid(np.arange(16), np.arange(2), np.arange(2), np.arange(4), indexing="ij")
    peer, part, low, level = (a.reshape(-1)[:, None] for a in rows)
    columns = np.meshgrid(np.arange(2), np.arange(2), np.arange(64), indexing="ij")
    out_part, out_low, kz = (a.reshape(-1)[None, :] for a in columns)
    angle = 2 * np.pi * ((4 * peer + level) * kz % NZ) / NZ
    cross = np.where(out_part == 0, np.sin(angle), -np.sin(angle))
    table = np.where(out_part == part, np.cos(angle), cross) * (low == out_low)
    return halves(table.astype(np.float32))


def quarter(a, b, c, d):
    (ar, ai), (br, bi), (cr, ci), (dr, di) = a, b, c, d
    s0r, s0i, s1r, s1i = ar + cr, ai + ci, ar - cr, ai - ci
    s2r, s2i, s3r, s3i = br + dr, bi + di, br - dr, bi - di
    return (
        (s0r + s2r, s0i + s2i),
        (s1r + s3i, s1i - s3r),
        (s0r - s2r, s0i - s2i),
        (s1r - s3i, s1i + s3r),
    )


def turn(value, numerator, denominator):
    re, im = value
    step = numerator % denominator
    if step == 0:
        return value
    if 4 * step == denominator:
        return (im, -re)
    if 8 * step == denominator:
        root = math.sqrt(0.5)
        return ((re + im) * root, (im - re) * root)
    if 8 * step == 3 * denominator:
        root = math.sqrt(0.5)
        return ((im - re) * root, -(re + im) * root)
    c = math.cos(2 * math.pi * step / denominator)
    s = math.sin(2 * math.pi * step / denominator)
    return (re * c + im * s, im * c - re * s)


def transform16(values):
    inner = [quarter(values[n], values[4 + n], values[8 + n], values[12 + n]) for n in range(4)]
    out = [None] * 16
    for k1 in range(4):
        column = [turn(inner[n][k1], n * k1, 16) for n in range(4)]
        for k2, value in enumerate(quarter(*column)):
            out[k1 + 4 * k2] = value
    return out


def split(value):
    high = value.astype(BF16)
    return high, (value - high.astype(F32)).astype(BF16)


def dot(a, b, dims):
    return lax.dot_general(a, b, dims, preferred_element_type=F32)


def cosine_of_turns(steps, period):
    turns = steps * (1.0 / period)
    turns = turns - jnp.floor(turns)
    s = (0.25 - jnp.abs(turns - 0.5)) * (2.0 * math.pi)
    s2 = s * s
    poly = 1.0 / 6227020800.0
    for c in (-1.0 / 39916800.0, 1.0 / 362880.0, -1.0 / 5040.0, 1.0 / 120.0, -1.0 / 6.0, 1.0):
        poly = poly * s2 + c
    return -(poly * s)


def exchange_kernel(
    field, modes_in, x_tab, y_tab, y_twid, z_tab,
    levels_out, local_out, z_t,
    cells, modes, x_t, y_t, tw, cells_parts, lines, blocks, y_parts, waves, phases, chosen,
    coef_one, coef_mine, coef_col, coef_row, coef_sum, coef_all,
    load_sem, row_send, row_recv, col_send, col_recv,
    small_send, small_recv,
):
    row, col = lax.axis_index("row"), lax.axis_index("col")
    z_at, y_lo = lax.rem(row, 8), row // 8

    def row_peer(k):
        return lax.rem(z_at + k, 8) + 8 * lax.rem(y_lo + k // 8, 2)

    def col_peer(k):
        return lax.rem(col + k, PEERS)

    barrier = pltpu.get_barrier_semaphore()

    @pl.loop(1, PEERS)
    def _(k):
        pl.semaphore_signal(barrier, inc=1, device_id={"row": row_peer(k)}, device_id_type=MESH)
        pl.semaphore_signal(barrier, inc=1, device_id={"col": col_peer(k)}, device_id_type=MESH)

    pieces = [(x_tab, x_t)] + [(field.at[:, pl.ds(128 * t, 128)], cells.at[t]) for t in range(NX // 128)]
    first_pieces = len(pieces)
    pieces += [(modes_in, modes), (y_twid, tw), (y_tab, y_t), (z_tab, z_t)]
    loads = [pltpu.make_async_copy(source, target, load_sem.at[i]) for i, (source, target) in enumerate(pieces)]
    for each in loads:
        each.start()

    def row_copy(chunk, peer):
        return pltpu.make_async_remote_copy(
            src_ref=lines.at[chunk, peer], dst_ref=blocks.at[chunk, row],
            send_sem=row_send.at[chunk], recv_sem=row_recv.at[chunk],
            device_id={"row": peer}, device_id_type=MESH,
        )

    def col_copy(chunk, k):
        peer = col_peer(k)
        return pltpu.make_async_remote_copy(
            src_ref=waves.at[chunk, peer], dst_ref=levels_out.at[chunk, col],
            send_sem=col_send.at[chunk], recv_sem=col_recv.at[chunk],
            device_id={"col": peer}, device_id_type=MESH,
        )

    def wait_bytes(ref, sem):
        pltpu.make_async_copy(ref, ref, sem).wait()

    def send_rows(slot):
        for plane, lead in zip(PLANES, LEAD):
            chunk = slot + lead
            there = jnp.logical_and(chunk >= 0, chunk < CHUNKS)
            for peer in (plane, 8 + plane):

                @pl.when(jnp.logical_and(there, peer != row))
                def _(chunk=chunk, peer=peer):
                    row_copy(chunk, peer).start()

    for each in loads[:first_pieces]:
        each.wait()
    def x_transform(member):
        for t in range(NX // 128):
            high, low = split(cells[t, pl.ds(member, ROWS * LEVELS, stride=MEMBERS), :])
            lanes = pl.ds(t * 128, 128)
            cells_parts[pl.ds(0, 128), lanes], cells_parts[pl.ds(128, 128), lanes] = high, low
        for half in range(2):
            chunk = member * 2 + half
            table = pl.ds(half * 256, 256)
            both = dot(x_t[0, table], cells_parts[...], NT)
            value = both[:, :128] + both[:, 128:] + dot(x_t[1, table], cells_parts[pl.ds(0, 128)], NT)
            lines[chunk] = value.reshape(PEERS, 16, 128)
            blocks[chunk, row] = lines[chunk, row]

    x_transform(0)
    pl.semaphore_wait(barrier, 2 * (PEERS - 1))
    for slot in range(-max(LEAD), 1):
        send_rows(slot)

    @pl.loop(1, MEMBERS)
    def _(member):
        x_transform(member)

        @pl.when(member <= AHEAD // 2)
        def _():
            send_rows(2 * member - 1)

        @pl.when(member < AHEAD // 2)
        def _():
            send_rows(2 * member)

    for each in loads[first_pieces:]:
        each.wait()

    def mode_row(i):
        return modes[i : i + 1, :].astype(F32)

    def down(value):
        return jnp.broadcast_to(value, (128, MODES)).T

    kx = mode_row(0)
    block = jnp.floor(kx * (1.0 / 16.0))
    half = jnp.floor((kx - 16.0 * block) * 0.125)
    place = half * 256.0 + block * 16.0 + (kx - 16.0 * block - 8.0 * half)
    place = down(place)
    lane = lax.broadcasted_iota(jnp.int32, (MODES, 128), 1)
    lane_f = lane.astype(F32)
    choose = jnp.concatenate(
        [
            jnp.concatenate([(place + 8.0 * part == lane_f + 128.0 * t).astype(F32) for t in range(4)], axis=1)
            for part in range(2)
        ],
        axis=0,
    ).astype(BF16)
    cell = (lane // 4).astype(F32) + (row * ROWS).astype(F32)
    level = lax.rem(lane, 4).astype(F32) + (col * LEVELS).astype(F32)
    steps = down(mode_row(1)) * cell + down(mode_row(2)) * level * float(NY // NZ)
    cos = cosine_of_turns(steps, float(NY))
    sin = cosine_of_turns(steps - 128.0, float(NY))
    phases[0], phases[1] = cos, sin
    chosen[...] = choose
    own_member = lax.broadcasted_iota(jnp.int32, (8, 128), 0)

    def add_member(member, coef):
        here = (own_member == member).astype(F32).astype(BF16)
        high, low = split(lines[pl.ds(2 * member, 2)].reshape(512, 128))
        both = dot(chosen[...], jnp.concatenate([high, low], axis=1), NN)
        at_modes = both[:, :128] + both[:, 128:]
        re, im = at_modes[:MODES], at_modes[MODES:]
        cos, sin = phases[0], phases[1]
        value = jnp.concatenate([re * cos + im * sin, im * cos - re * sin], axis=0)
        high, low = split(value)
        return coef + dot(here, high, NT) + dot(here, low, NT)

    coef = lax.fori_loop(0, MEMBERS, add_member, jnp.zeros((8, 2 * MODES), F32))
    for t in range(4):
        coef_one[t] = coef[:, 128 * t : 128 * t + 128]

    def tile_copy(k):
        peer = col_peer(k)
        return pltpu.make_async_remote_copy(
            src_ref=coef_one.at[lax.rem(peer, 4)], dst_ref=coef_col.at[col],
            send_sem=small_send.at[0], recv_sem=small_recv.at[0], device_id={"col": peer}, device_id_type=MESH,
        )

    def sum_copy(k):
        return pltpu.make_async_remote_copy(
            src_ref=coef_mine, dst_ref=coef_row.at[row],
            send_sem=small_send.at[1], recv_sem=small_recv.at[1], device_id={"row": row_peer(k)}, device_id_type=MESH,
        )

    def share_copy(k):
        peer = (col // 4) * 4 + lax.rem(col + k, 4)
        return pltpu.make_async_remote_copy(
            src_ref=coef_sum, dst_ref=coef_all.at[lax.rem(col, 4)],
            send_sem=small_send.at[2], recv_sem=small_recv.at[2], device_id={"col": peer}, device_id_type=MESH,
        )

    def start_all(copy, count):
        @pl.loop(1, count)
        def _(k):
            copy(k).start()

    coef_col[col] = coef_one[lax.rem(col, 4)]
    start_all(tile_copy, PEERS)

    def small_step(step):
        if step == 0:
            wait_bytes(coef_col.at[pl.ds(0, PEERS - 1)], small_recv.at[0])
            total = coef_col[0]
            for i in range(1, PEERS):
                total = total + coef_col[i]
            coef_mine[...] = total
            coef_row[row] = total
            start_all(sum_copy, PEERS)
        elif step == 1:
            wait_bytes(coef_row.at[pl.ds(0, PEERS - 1)], small_recv.at[1])
            total = coef_row[0]
            for i in range(1, PEERS):
                total = total + coef_row[i]
            coef_sum[...] = total
            coef_all[lax.rem(col, 4)] = total
            start_all(share_copy, 4)
        else:
            wait_bytes(coef_all.at[pl.ds(0, 3)], small_recv.at[2])
            coef = jnp.concatenate([coef_all[i] for i in range(4)], axis=1)
            anomaly = coef - jnp.mean(coef, axis=0, keepdims=True)
            turned = anomaly.T
            a_high, a_low = split(turned)
            b_high, b_low = split(anomaly)
            kx, ky, kz = mode_row(0), mode_row(1), mode_row(2)
            ky = jnp.where(ky < NY // 2, ky, ky - NY)
            kz = jnp.where(kz < NZ // 2, kz, kz - NZ)
            dist = jnp.zeros((MODES, MODES), F32)
            for wave in (kx, ky, kz):
                tall = down(wave)
                tall = jnp.concatenate([tall, tall], axis=1)
                dist += (tall - wave) ** 2
            taper = jnp.exp(-dist * (1.0 / (2.0 * REACH * REACH))) * (1.0 / (MEMBERS - 1))
            for i in range(2):
                at = slice(i * MODES, (i + 1) * MODES)
                cov = dot(a_high[at], b_high, NN) + dot(a_high[at], b_low, NN) + dot(a_low[at], b_high, NN)
                local_out[at, :MODES] = cov[:, :MODES] * taper
                local_out[at, MODES:] = cov[:, MODES:] * taper

    @pl.loop(0, CHUNKS)
    def _(chunk):
        send_rows(chunk + AHEAD)

        wait_bytes(blocks.at[chunk, pl.ds(0, PEERS - 1)], row_recv.at[chunk])
        out = transform16([(blocks[chunk, i, 0:8, :], blocks[chunk, i, 8:16, :]) for i in range(16)])
        for pair in range(8):
            parts = []
            for k1 in (2 * pair, 2 * pair + 1):
                re, im = out[k1]
                if k1 > 0:
                    c = tw[2 * k1 : 2 * k1 + 1, :]
                    s = tw[2 * k1 + 1 : 2 * k1 + 2, :]
                    re, im = re * c + im * s, im * c - re * s
                parts.append((re, im))
            for part in range(2):
                high, low = split(jnp.concatenate([parts[0][part], parts[1][part]], axis=0))
                at = pl.ds(part * 128, 128)
                y_parts[pl.ds(16 * pair, 16), at] = high
                y_parts[pl.ds(128 + 16 * pair, 16), at] = low
        both = dot(y_t[0], y_parts[...], NT)
        value = both[:, :128] + both[:, 128:] + dot(y_t[1], y_parts[pl.ds(0, 128)], NT)
        waves[chunk] = value.reshape(PEERS, 16, 128)

        for k in range(1, PEERS):
            col_copy(chunk, k).start()

        levels_out[chunk, col] = waves[chunk, col]

        for step, at in enumerate((2, 6, 10)):
            @pl.when(chunk == at)
            def _(step=step):
                small_step(step)

    wait_bytes(coef_col.at[pl.ds(0, PEERS - 1)], small_send.at[0])
    wait_bytes(coef_row.at[pl.ds(0, PEERS - 1)], small_send.at[1])
    wait_bytes(coef_all.at[pl.ds(0, 3)], small_send.at[2])

    @pl.loop(0, CHUNKS)
    def _(chunk):
        wait_bytes(lines.at[chunk, pl.ds(0, PEERS - 1)], row_send.at[chunk])
        wait_bytes(waves.at[chunk, pl.ds(0, PEERS - 1)], col_send.at[chunk])
        wait_bytes(levels_out.at[chunk, pl.ds(0, PEERS - 1)], col_recv.at[chunk])


def exchange(field, modes):
    any_space = pl.BlockSpec(memory_space=pl.ANY)
    dma = pltpu.SemaphoreType.DMA
    return pl.pallas_call(
        exchange_kernel,
        out_shape=(
            pltpu.VMEM((CHUNKS, PEERS, 16, 128), F32),
            pltpu.VMEM((2 * MODES, 2 * MODES), F32),
            pltpu.VMEM((2, 256, 256), BF16),
        ),
        in_specs=[any_space] * 6,
        out_specs=(pl.BlockSpec(memory_space=pltpu.VMEM),) * 3,
        scratch_shapes=[
            pltpu.VMEM((NX // 128, ROWS * LEVELS * MEMBERS, 128), F32),
            pltpu.VMEM((3, MODES), jnp.int32),
            pltpu.VMEM((2, 512, 512), BF16),
            pltpu.VMEM((2, 256, 256), BF16),
            pltpu.VMEM((32, 128), F32),
            pltpu.VMEM((256, NX), BF16),
            pltpu.VMEM((CHUNKS, PEERS, 16, 128), F32),
            pltpu.VMEM((CHUNKS, PEERS, 16, 128), F32),
            pltpu.VMEM((256, 256), BF16),
            pltpu.VMEM((CHUNKS, PEERS, 16, 128), F32),
            pltpu.VMEM((2, MODES, 128), F32),
            pltpu.VMEM((512, 512), BF16),
            pltpu.VMEM((4, 8, 128), F32),
            pltpu.VMEM((8, 128), F32),
            pltpu.VMEM((PEERS, 8, 128), F32),
            pltpu.VMEM((PEERS, 8, 128), F32),
            pltpu.VMEM((8, 128), F32),
            pltpu.VMEM((4, 8, 128), F32),
            dma((9,)),
            dma((CHUNKS,)),
            dma((CHUNKS,)),
            dma((CHUNKS,)),
            dma((CHUNKS,)),
            dma((3,)),
            dma((3,)),
        ],
        compiler_params=pltpu.CompilerParams(collective_id=0, has_side_effects=True, vmem_limit_bytes=VMEM),
        cost_estimate=pl.CostEstimate(flops=10**10, bytes_accessed=8 << 20, transcendentals=0),
        name="exchange",
    )(field.reshape(-1, NX), modes, x_table(), y_table(), y_twiddle(), z_table())


def levels_kernel(levels, table, local_in, spectrum, local, rows, ready, out_sem, local_sem):
    local_copy = pltpu.make_async_copy(local_in, local, local_sem)
    local_copy.start()
    copies = []
    for member in range(MEMBERS):
        for half in range(2):
            high, low = split(levels[2 * member + half].reshape(256, 128).T)
            out = dot(high, table[0], NN) + dot(high, table[1], NN) + dot(low, table[0], NN)
            for k1 in range(16):
                for part in range(2):
                    at = member * 512 + k1 * 32 + 16 * half + part
                    rows[pl.ds(at, 8, stride=2), :] = out[8 * k1 : 8 * k1 + 8, 128 * part : 128 * part + 128]
        value = rows[pl.ds(member * 512, 512), :].reshape(16, 32, 128)
        for low_k in range(2):
            ready[pl.ds(low_k * 16, 16), member] = value[:, :, low_k * NZ : (low_k + 1) * NZ]
        copies.append(pltpu.make_async_copy(ready.at[:, member], spectrum.at[:, member], out_sem.at[member]))
        copies[-1].start()
    for copy in copies:
        copy.wait()
    local_copy.wait()


def from_levels(levels, local, table):
    here = pl.BlockSpec(memory_space=pltpu.VMEM)
    any_space = pl.BlockSpec(memory_space=pl.ANY)
    spectrum, local = pl.pallas_call(
        levels_kernel,
        out_shape=(
            jax.ShapeDtypeStruct((NY // PEERS, MEMBERS, 32, NZ), F32),
            jax.ShapeDtypeStruct((2 * MODES, 2 * MODES), F32),
        ),
        in_specs=[here] * 3,
        out_specs=(any_space, any_space),
        scratch_shapes=[
            pltpu.VMEM((MEMBERS * 512, 128), F32),
            pltpu.VMEM((NY // PEERS, MEMBERS, 32, NZ), F32),
            pltpu.SemaphoreType.DMA((MEMBERS,)),
            pltpu.SemaphoreType.DMA,
        ],
        compiler_params=pltpu.CompilerParams(vmem_limit_bytes=VMEM),
        cost_estimate=pl.CostEstimate(flops=10**9, bytes_accessed=8 << 20, transcendentals=0),
        name="from_levels",
    )(*(pltpu.with_memory_space_constraint(each, pltpu.VMEM) for each in (levels, table, local)))
    return jnp.transpose(spectrum, (3, 0, 1, 2)), local


def per_device(field, modes):
    return from_levels(*exchange(field, modes))


def solution(mesh):
    return jax.shard_map(
        per_device,
        mesh=mesh,
        in_specs=(P("row", "col", None, None), P()),
        out_specs=(P(None, "col", None, "row"), P()),
        check_vma=False,
    )
```

```python
import functools
import math

import jax
import jax.numpy as jnp
import numpy as np
from jax import lax
from jax.experimental import pallas as pl
from jax.experimental.pallas import tpu as pltpu
from jax.sharding import PartitionSpec as P

NX, NY, NZ, MEMBERS, MODES, REACH = 512, 512, 64, 8, 256, 64
PEERS = 16
LEVELS = NZ // PEERS
ROWS = NY // PEERS
CHUNKS = 2 * MEMBERS
AHEAD = 4
DONE = MEMBERS - 1
PLANES = (0, 1, 2, 3, 7, 6, 4, 5)
LEAD = (1, 0, 0, 0, 0, 0, 0, 0)
VMEM = 67_043_328 - (7 << 20) - (256 << 10)
F32, BF16 = jnp.float32, jnp.bfloat16
MESH = pl.DeviceIdType.MESH
NT = (((1,), (1,)), ((), ()))
NN = (((1,), (0,)), ((), ()))


def halves(table):
    high = table.astype(jnp.bfloat16)
    low = (table - high.astype(np.float32)).astype(jnp.bfloat16)
    return np.stack([high, low])


@functools.cache
def x_table():
    half, block, part, wave = np.meshgrid(np.arange(2), np.arange(16), np.arange(2), np.arange(8), indexing="ij")
    kx = (block * 16 + half * 8 + wave).reshape(-1)
    part = part.reshape(-1)
    angle = 2 * np.pi * (kx[:, None] * np.arange(NX)[None, :] % NX) / NX
    table = np.where(part[:, None] == 0, np.cos(angle), -np.sin(angle)) / math.sqrt(NX * NY * NZ)
    return halves(table.astype(np.float32))


@functools.cache
def y_table():
    rows = np.meshgrid(np.arange(16), np.arange(2), np.arange(2), np.arange(4), indexing="ij")
    peer, out_part, low, out_level = (a.reshape(-1)[:, None] for a in rows)
    columns = np.meshgrid(np.arange(2), np.arange(32), np.arange(4), indexing="ij")
    part, cell, level = (a.reshape(-1)[None, :] for a in columns)
    angle = 2 * np.pi * (cell * (peer * 2 + low) % 32) / 32
    cross = np.where(out_part == 0, np.sin(angle), -np.sin(angle))
    table = np.where(out_part == part, np.cos(angle), cross) * (level == out_level)
    return halves(table.astype(np.float32))


@functools.cache
def y_twiddle():
    k1 = np.arange(16)[:, None]
    cell = (np.arange(128) // 4)[None, :]
    angle = 2 * np.pi * k1 * cell / NY
    return np.stack([np.cos(angle), np.sin(angle)], axis=1).reshape(32, 128).astype(np.float32)


@functools.cache
def z_table():
    rows = np.meshgrid(np.arange(16), np.arange(2), np.arange(2), np.arange(4), indexing="ij")
    peer, part, low, level = (a.reshape(-1)[:, None] for a in rows)
    columns = np.meshgrid(np.arange(2), np.arange(2), np.arange(64), indexing="ij")
    out_part, out_low, kz = (a.reshape(-1)[None, :] for a in columns)
    angle = 2 * np.pi * ((4 * peer + level) * kz % NZ) / NZ
    cross = np.where(out_part == 0, np.sin(angle), -np.sin(angle))
    table = np.where(out_part == part, np.cos(angle), cross) * (low == out_low)
    return halves(table.astype(np.float32))


def quarter(a, b, c, d):
    (ar, ai), (br, bi), (cr, ci), (dr, di) = a, b, c, d
    s0r, s0i, s1r, s1i = ar + cr, ai + ci, ar - cr, ai - ci
    s2r, s2i, s3r, s3i = br + dr, bi + di, br - dr, bi - di
    return (
        (s0r + s2r, s0i + s2i),
        (s1r + s3i, s1i - s3r),
        (s0r - s2r, s0i - s2i),
        (s1r - s3i, s1i + s3r),
    )


def turn(value, numerator, denominator):
    re, im = value
    step = numerator % denominator
    if step == 0:
        return value
    if 4 * step == denominator:
        return (im, -re)
    if 8 * step == denominator:
        root = math.sqrt(0.5)
        return ((re + im) * root, (im - re) * root)
    if 8 * step == 3 * denominator:
        root = math.sqrt(0.5)
        return ((im - re) * root, -(re + im) * root)
    c = math.cos(2 * math.pi * step / denominator)
    s = math.sin(2 * math.pi * step / denominator)
    return (re * c + im * s, im * c - re * s)


def transform16(values):
    inner = [quarter(values[n], values[4 + n], values[8 + n], values[12 + n]) for n in range(4)]
    out = [None] * 16
    for k1 in range(4):
        column = [turn(inner[n][k1], n * k1, 16) for n in range(4)]
        for k2, value in enumerate(quarter(*column)):
            out[k1 + 4 * k2] = value
    return out


def split(value):
    high = value.astype(BF16)
    return high, (value - high.astype(F32)).astype(BF16)


def dot(a, b, dims):
    return lax.dot_general(a, b, dims, preferred_element_type=F32)


def cosine_of_turns(steps, period):
    turns = steps * (1.0 / period)
    turns = turns - jnp.floor(turns)
    s = (0.25 - jnp.abs(turns - 0.5)) * (2.0 * math.pi)
    s2 = s * s
    poly = 1.0 / 6227020800.0
    for c in (-1.0 / 39916800.0, 1.0 / 362880.0, -1.0 / 5040.0, 1.0 / 120.0, -1.0 / 6.0, 1.0):
        poly = poly * s2 + c
    return -(poly * s)


def z_transform(levels, table, rows, ready, member):
    for half in range(2):
        high, low = split(levels[2 * member + half].reshape(256, 128).T)
        out = dot(high, table[0], NN) + dot(high, table[1], NN) + dot(low, table[0], NN)
        for k1 in range(16):
            for part in range(2):
                at = k1 * 32 + 16 * half + part
                rows[pl.ds(at, 8, stride=2), :] = out[8 * k1 : 8 * k1 + 8, 128 * part : 128 * part + 128]
    value = rows[...].reshape(16, 32, 128)
    for low_k in range(2):
        ready[pl.ds(low_k * 16, 16)] = value[:, :, low_k * NZ : (low_k + 1) * NZ]


def exchange_kernel(
    field, modes_in, x_tab, y_tab, y_twid, z_tab,
    levels_out, local_out, z_t, ready,
    cells, modes, x_t, y_t, tw, cells_parts, lines, blocks, y_parts, waves, phases, chosen, z_rows,
    coef_one, coef_mine, coef_col, coef_row, coef_sum, coef_all,
    load_sem, row_send, row_recv, col_send, col_recv,
    small_send, small_recv,
):
    row, col = lax.axis_index("row"), lax.axis_index("col")
    z_at, y_lo = lax.rem(row, 8), row // 8

    def row_peer(k):
        return lax.rem(z_at + k, 8) + 8 * lax.rem(y_lo + k // 8, 2)

    x_at, y_hi, core = col // 4, lax.rem(col // 2, 2), lax.rem(col, 2)

    def col_peer(k):
        x_step, y_step, core_step = (2, 1, 3, 0)[(k - 1) // 4], 1 - ((k - 1) // 2) % 2, k % 2
        return lax.rem(x_at + x_step, 4) * 4 + lax.rem(y_hi + y_step, 2) * 2 + lax.rem(core + core_step, 2)

    barrier = pltpu.get_barrier_semaphore()

    @pl.loop(1, PEERS)
    def _(k):
        pl.semaphore_signal(barrier, inc=1, device_id={"row": row_peer(k)}, device_id_type=MESH)
        pl.semaphore_signal(barrier, inc=1, device_id={"col": lax.rem(col + k, PEERS)}, device_id_type=MESH)

    pieces = [(x_tab, x_t)] + [(field.at[:, pl.ds(128 * t, 128)], cells.at[t]) for t in range(NX // 128)]
    first_pieces = len(pieces)
    pieces += [(modes_in, modes), (y_twid, tw), (y_tab, y_t), (z_tab, z_t)]
    loads = [pltpu.make_async_copy(source, target, load_sem.at[i]) for i, (source, target) in enumerate(pieces)]
    for each in loads:
        each.start()

    def row_copy(chunk, peer):
        return pltpu.make_async_remote_copy(
            src_ref=lines.at[chunk, peer], dst_ref=blocks.at[chunk, row],
            send_sem=row_send.at[chunk], recv_sem=row_recv.at[chunk],
            device_id={"row": peer}, device_id_type=MESH,
        )

    def col_copy(chunk, k):
        peer = col_peer(k)
        return pltpu.make_async_remote_copy(
            src_ref=waves.at[chunk, peer], dst_ref=levels_out.at[chunk, col],
            send_sem=col_send.at[chunk], recv_sem=col_recv.at[chunk],
            device_id={"col": peer}, device_id_type=MESH,
        )

    def wait_bytes(ref, sem):
        pltpu.make_async_copy(ref, ref, sem).wait()

    def send_rows(slot):
        for plane, lead in zip(PLANES, LEAD):
            chunk = slot + lead
            there = jnp.logical_and(chunk >= 0, chunk < CHUNKS)
            for peer in (plane, 8 + plane):

                @pl.when(jnp.logical_and(there, peer != row))
                def _(chunk=chunk, peer=peer):
                    row_copy(chunk, peer).start()

    for each in loads[:first_pieces]:
        each.wait()
    def x_transform(member):
        for t in range(NX // 128):
            high, low = split(cells[t, pl.ds(member, ROWS * LEVELS, stride=MEMBERS), :])
            lanes = pl.ds(t * 128, 128)
            cells_parts[pl.ds(0, 128), lanes], cells_parts[pl.ds(128, 128), lanes] = high, low
        for half in range(2):
            chunk = member * 2 + half
            table = pl.ds(half * 256, 256)
            both = dot(x_t[0, table], cells_parts[...], NT)
            value = both[:, :128] + both[:, 128:] + dot(x_t[1, table], cells_parts[pl.ds(0, 128)], NT)
            lines[chunk] = value.reshape(PEERS, 16, 128)
            blocks[chunk, row] = lines[chunk, row]

    x_transform(0)
    pl.semaphore_wait(barrier, 2 * (PEERS - 1))
    for slot in range(-max(LEAD), 1):
        send_rows(slot)

    @pl.loop(1, MEMBERS)
    def _(member):
        x_transform(member)

        @pl.when(member <= AHEAD // 2)
        def _():
            send_rows(2 * member - 1)

        @pl.when(member < AHEAD // 2)
        def _():
            send_rows(2 * member)

    for each in loads[first_pieces:]:
        each.wait()

    def mode_row(i):
        return modes[i : i + 1, :].astype(F32)

    def down(value):
        return jnp.broadcast_to(value, (128, MODES)).T

    kx = mode_row(0)
    block = jnp.floor(kx * (1.0 / 16.0))
    half = jnp.floor((kx - 16.0 * block) * 0.125)
    place = half * 256.0 + block * 16.0 + (kx - 16.0 * block - 8.0 * half)
    place = down(place)
    lane = lax.broadcasted_iota(jnp.int32, (MODES, 128), 1)
    lane_f = lane.astype(F32)
    choose = jnp.concatenate(
        [
            jnp.concatenate([(place + 8.0 * part == lane_f + 128.0 * t).astype(F32) for t in range(4)], axis=1)
            for part in range(2)
        ],
        axis=0,
    ).astype(BF16)
    cell = (lane // 4).astype(F32) + (row * ROWS).astype(F32)
    level = lax.rem(lane, 4).astype(F32) + (col * LEVELS).astype(F32)
    steps = down(mode_row(1)) * cell + down(mode_row(2)) * level * float(NY // NZ)
    cos = cosine_of_turns(steps, float(NY))
    sin = cosine_of_turns(steps - 128.0, float(NY))
    phases[0], phases[1] = cos, sin
    chosen[...] = choose
    own_member = lax.broadcasted_iota(jnp.int32, (8, 128), 0)

    def add_member(member, coef):
        here = (own_member == member).astype(F32).astype(BF16)
        high, low = split(lines[pl.ds(2 * member, 2)].reshape(512, 128))
        both = dot(chosen[...], jnp.concatenate([high, low], axis=1), NN)
        at_modes = both[:, :128] + both[:, 128:]
        re, im = at_modes[:MODES], at_modes[MODES:]
        cos, sin = phases[0], phases[1]
        value = jnp.concatenate([re * cos + im * sin, im * cos - re * sin], axis=0)
        high, low = split(value)
        return coef + dot(here, high, NT) + dot(here, low, NT)

    coef = lax.fori_loop(0, MEMBERS, add_member, jnp.zeros((8, 2 * MODES), F32))
    for t in range(4):
        for pair in range(4):
            coef_one[4 * t + pair] = coef[2 * pair : 2 * pair + 2, 128 * t : 128 * t + 128]

    def piece_copy(k):
        peer = col_peer(k)
        return pltpu.make_async_remote_copy(
            src_ref=coef_one.at[peer], dst_ref=coef_col.at[col],
            send_sem=small_send.at[0], recv_sem=small_recv.at[0], device_id={"col": peer}, device_id_type=MESH,
        )

    def sum_copy(k):
        return pltpu.make_async_remote_copy(
            src_ref=coef_mine, dst_ref=coef_row.at[row],
            send_sem=small_send.at[1], recv_sem=small_recv.at[1], device_id={"row": row_peer(k)}, device_id_type=MESH,
        )

    def share_copy(k):
        return pltpu.make_async_remote_copy(
            src_ref=coef_sum, dst_ref=coef_all.at[col],
            send_sem=small_send.at[2], recv_sem=small_recv.at[2], device_id={"col": col_peer(k)}, device_id_type=MESH,
        )

    def start_all(copy):
        for k in range(1, PEERS):
            copy(k).start()

    coef_col[col] = coef_one[col]
    start_all(piece_copy)

    def small_step(step):
        if step == 0:
            wait_bytes(coef_col.at[pl.ds(0, PEERS - 1)], small_recv.at[0])
            total = coef_col[0]
            for i in range(1, PEERS):
                total = total + coef_col[i]
            coef_mine[...] = total
            coef_row[row] = total
            start_all(sum_copy)
        elif step == 1:
            wait_bytes(coef_row.at[pl.ds(0, PEERS - 1)], small_recv.at[1])
            total = coef_row[0]
            for i in range(1, PEERS):
                total = total + coef_row[i]
            coef_sum[...] = total
            coef_all[col] = total
            start_all(share_copy)
        else:
            wait_bytes(coef_all.at[pl.ds(0, PEERS - 1)], small_recv.at[2])
            tiles = [jnp.concatenate([coef_all[4 * t + pair] for pair in range(4)], axis=0) for t in range(4)]
            coef = jnp.concatenate(tiles, axis=1)
            anomaly = coef - jnp.mean(coef, axis=0, keepdims=True)
            turned = anomaly.T
            a_high, a_low = split(turned)
            b_high, b_low = split(anomaly)
            kx, ky, kz = mode_row(0), mode_row(1), mode_row(2)
            ky = jnp.where(ky < NY // 2, ky, ky - NY)
            kz = jnp.where(kz < NZ // 2, kz, kz - NZ)
            dist = jnp.zeros((MODES, MODES), F32)
            for wave in (kx, ky, kz):
                tall = down(wave)
                tall = jnp.concatenate([tall, tall], axis=1)
                dist += (tall - wave) ** 2
            taper = jnp.exp(-dist * (1.0 / (2.0 * REACH * REACH))) * (1.0 / (MEMBERS - 1))
            for i in range(2):
                at = slice(i * MODES, (i + 1) * MODES)
                cov = dot(a_high[at], b_high, NN) + dot(a_high[at], b_low, NN) + dot(a_low[at], b_high, NN)
                local_out[at, :MODES] = cov[:, :MODES] * taper
                local_out[at, MODES:] = cov[:, MODES:] * taper

    @pl.loop(0, CHUNKS)
    def _(chunk):
        send_rows(chunk + AHEAD)

        wait_bytes(blocks.at[chunk, pl.ds(0, PEERS - 1)], row_recv.at[chunk])
        out = transform16([(blocks[chunk, i, 0:8, :], blocks[chunk, i, 8:16, :]) for i in range(16)])
        for pair in range(8):
            parts = []
            for k1 in (2 * pair, 2 * pair + 1):
                re, im = out[k1]
                if k1 > 0:
                    c = tw[2 * k1 : 2 * k1 + 1, :]
                    s = tw[2 * k1 + 1 : 2 * k1 + 2, :]
                    re, im = re * c + im * s, im * c - re * s
                parts.append((re, im))
            for part in range(2):
                high, low = split(jnp.concatenate([parts[0][part], parts[1][part]], axis=0))
                at = pl.ds(part * 128, 128)
                y_parts[pl.ds(16 * pair, 16), at] = high
                y_parts[pl.ds(128 + 16 * pair, 16), at] = low
        both = dot(y_t[0], y_parts[...], NT)
        value = both[:, :128] + both[:, 128:] + dot(y_t[1], y_parts[pl.ds(0, 128)], NT)
        waves[chunk] = value.reshape(PEERS, 16, 128)

        for k in range(1, PEERS):
            col_copy(chunk, k).start()

        levels_out[chunk, col] = waves[chunk, col]

        for step, at in enumerate((4, 9)):
            @pl.when(chunk == at)
            def _(step=step):
                small_step(step)

    small_step(2)

    def wait_levels(member):
        for chunk in (2 * member, 2 * member + 1):
            wait_bytes(levels_out.at[chunk, pl.ds(0, PEERS - 1)], col_recv.at[chunk])

    @pl.loop(0, DONE)
    def _(member):
        wait_levels(member)
        z_transform(levels_out, z_t, z_rows, ready.at[member], member)

    for member in range(DONE, MEMBERS):
        wait_levels(member)
    wait_bytes(coef_col.at[pl.ds(0, PEERS - 1)], small_send.at[0])
    wait_bytes(coef_row.at[pl.ds(0, PEERS - 1)], small_send.at[1])
    wait_bytes(coef_all.at[pl.ds(0, PEERS - 1)], small_send.at[2])

    @pl.loop(0, CHUNKS)
    def _(chunk):
        wait_bytes(lines.at[chunk, pl.ds(0, PEERS - 1)], row_send.at[chunk])
        wait_bytes(waves.at[chunk, pl.ds(0, PEERS - 1)], col_send.at[chunk])


def exchange(field, modes):
    any_space = pl.BlockSpec(memory_space=pl.ANY)
    dma = pltpu.SemaphoreType.DMA
    return pl.pallas_call(
        exchange_kernel,
        out_shape=(
            pltpu.VMEM((CHUNKS, PEERS, 16, 128), F32),
            pltpu.VMEM((2 * MODES, 2 * MODES), F32),
            pltpu.VMEM((2, 256, 256), BF16),
            pltpu.VMEM((MEMBERS, NY // PEERS, 32, NZ), F32),
        ),
        in_specs=[any_space] * 6,
        out_specs=(pl.BlockSpec(memory_space=pltpu.VMEM),) * 4,
        scratch_shapes=[
            pltpu.VMEM((NX // 128, ROWS * LEVELS * MEMBERS, 128), F32),
            pltpu.VMEM((3, MODES), jnp.int32),
            pltpu.VMEM((2, 512, 512), BF16),
            pltpu.VMEM((2, 256, 256), BF16),
            pltpu.VMEM((32, 128), F32),
            pltpu.VMEM((256, NX), BF16),
            pltpu.VMEM((CHUNKS, PEERS, 16, 128), F32),
            pltpu.VMEM((CHUNKS, PEERS, 16, 128), F32),
            pltpu.VMEM((256, 256), BF16),
            pltpu.VMEM((CHUNKS, PEERS, 16, 128), F32),
            pltpu.VMEM((2, MODES, 128), F32),
            pltpu.VMEM((512, 512), BF16),
            pltpu.VMEM((512, 128), F32),
            pltpu.VMEM((PEERS, 2, 128), F32),
            pltpu.VMEM((2, 128), F32),
            pltpu.VMEM((PEERS, 2, 128), F32),
            pltpu.VMEM((PEERS, 2, 128), F32),
            pltpu.VMEM((2, 128), F32),
            pltpu.VMEM((PEERS, 2, 128), F32),
            dma((9,)),
            dma((CHUNKS,)),
            dma((CHUNKS,)),
            dma((CHUNKS,)),
            dma((CHUNKS,)),
            dma((3,)),
            dma((3,)),
        ],
        compiler_params=pltpu.CompilerParams(collective_id=0, has_side_effects=True, vmem_limit_bytes=VMEM),
        cost_estimate=pl.CostEstimate(flops=10**10, bytes_accessed=8 << 20, transcendentals=0),
        name="exchange",
    )(field.reshape(-1, NX), modes, x_table(), y_table(), y_twiddle(), z_table())


def levels_kernel(levels, local_in, table, ready, spectrum, local, rows, last, out_sem, local_sem):
    copies = [pltpu.make_async_copy(local_in, local, local_sem)]
    for member in range(MEMBERS):
        source = ready.at[member] if member < DONE else last.at[member - DONE]
        copies.append(pltpu.make_async_copy(source, spectrum.at[:, member], out_sem.at[member]))
    for copy in copies[1 : DONE + 1]:
        copy.start()
    copies[0].start()
    for member in range(DONE, MEMBERS):
        z_transform(levels, table, rows, last.at[member - DONE], member)
        copies[member + 1].start()
    for copy in copies:
        copy.wait()


def from_levels(*parts):
    here = pl.BlockSpec(memory_space=pltpu.VMEM)
    any_space = pl.BlockSpec(memory_space=pl.ANY)
    spectrum, local = pl.pallas_call(
        levels_kernel,
        out_shape=(
            jax.ShapeDtypeStruct((NY // PEERS, MEMBERS, 32, NZ), F32),
            jax.ShapeDtypeStruct((2 * MODES, 2 * MODES), F32),
        ),
        in_specs=[here] * 4,
        out_specs=(any_space, any_space),
        scratch_shapes=[
            pltpu.VMEM((512, 128), F32),
            pltpu.VMEM((MEMBERS - DONE, NY // PEERS, 32, NZ), F32),
            pltpu.SemaphoreType.DMA((MEMBERS,)),
            pltpu.SemaphoreType.DMA,
        ],
        compiler_params=pltpu.CompilerParams(vmem_limit_bytes=VMEM),
        cost_estimate=pl.CostEstimate(flops=10**9, bytes_accessed=8 << 20, transcendentals=0),
        name="from_levels",
    )(*(pltpu.with_memory_space_constraint(each, pltpu.VMEM) for each in parts))
    return jnp.transpose(spectrum, (3, 0, 1, 2)), local


def per_device(field, modes):
    return from_levels(*exchange(field, modes))


def solution(mesh):
    return jax.shard_map(
        per_device,
        mesh=mesh,
        in_specs=(P("row", "col", None, None), P()),
        out_specs=(P(None, "col", None, "row"), P()),
        check_vma=False,
    )
```

```python
import functools
import math

import jax
import jax.numpy as jnp
import numpy as np
from jax import lax
from jax.experimental import pallas as pl
from jax.experimental.pallas import tpu as pltpu
from jax.sharding import PartitionSpec as P

NX, NY, NZ, MEMBERS, MODES, REACH = 512, 512, 64, 8, 256, 64
PEERS = 16
LEVELS = NZ // PEERS
ROWS = NY // PEERS
CHUNKS = 2 * MEMBERS
AHEAD = 4
DONE = MEMBERS - 1
PLANES = (0, 1, 2, 3, 7, 6, 4, 5)
LEAD = (2, 1, 1, 0, 0, 0, 0, 0)
VMEM = 67_043_328 - (7 << 20) - (256 << 10)
F32, BF16 = jnp.float32, jnp.bfloat16
MESH = pl.DeviceIdType.MESH
NT = (((1,), (1,)), ((), ()))
NN = (((1,), (0,)), ((), ()))


def halves(table):
    high = table.astype(jnp.bfloat16)
    low = (table - high.astype(np.float32)).astype(jnp.bfloat16)
    return np.stack([high, low])


@functools.cache
def x_table():
    half, block, part, wave = np.meshgrid(np.arange(2), np.arange(16), np.arange(2), np.arange(8), indexing="ij")
    kx = (block * 16 + half * 8 + wave).reshape(-1)
    part = part.reshape(-1)
    angle = 2 * np.pi * (kx[:, None] * np.arange(NX)[None, :] % NX) / NX
    table = np.where(part[:, None] == 0, np.cos(angle), -np.sin(angle)) / math.sqrt(NX * NY * NZ)
    return halves(table.astype(np.float32))


@functools.cache
def y_table():
    rows = np.meshgrid(np.arange(16), np.arange(2), np.arange(2), np.arange(4), indexing="ij")
    peer, out_part, low, out_level = (a.reshape(-1)[:, None] for a in rows)
    columns = np.meshgrid(np.arange(2), np.arange(32), np.arange(4), indexing="ij")
    part, cell, level = (a.reshape(-1)[None, :] for a in columns)
    angle = 2 * np.pi * (cell * (peer * 2 + low) % 32) / 32
    cross = np.where(out_part == 0, np.sin(angle), -np.sin(angle))
    table = np.where(out_part == part, np.cos(angle), cross) * (level == out_level)
    return halves(table.astype(np.float32))


@functools.cache
def y_twiddle():
    k1 = np.arange(16)[:, None]
    cell = (np.arange(128) // 4)[None, :]
    angle = 2 * np.pi * k1 * cell / NY
    return np.stack([np.cos(angle), np.sin(angle)], axis=1).reshape(32, 128).astype(np.float32)


@functools.cache
def z_table():
    rows = np.meshgrid(np.arange(16), np.arange(2), np.arange(2), np.arange(4), indexing="ij")
    peer, part, low, level = (a.reshape(-1)[:, None] for a in rows)
    columns = np.meshgrid(np.arange(2), np.arange(2), np.arange(64), indexing="ij")
    out_part, out_low, kz = (a.reshape(-1)[None, :] for a in columns)
    angle = 2 * np.pi * ((4 * peer + level) * kz % NZ) / NZ
    cross = np.where(out_part == 0, np.sin(angle), -np.sin(angle))
    table = np.where(out_part == part, np.cos(angle), cross) * (low == out_low)
    return halves(table.astype(np.float32))


def quarter(a, b, c, d):
    (ar, ai), (br, bi), (cr, ci), (dr, di) = a, b, c, d
    s0r, s0i, s1r, s1i = ar + cr, ai + ci, ar - cr, ai - ci
    s2r, s2i, s3r, s3i = br + dr, bi + di, br - dr, bi - di
    return (
        (s0r + s2r, s0i + s2i),
        (s1r + s3i, s1i - s3r),
        (s0r - s2r, s0i - s2i),
        (s1r - s3i, s1i + s3r),
    )


def turn(value, numerator, denominator):
    re, im = value
    step = numerator % denominator
    if step == 0:
        return value
    if 4 * step == denominator:
        return (im, -re)
    if 8 * step == denominator:
        root = math.sqrt(0.5)
        return ((re + im) * root, (im - re) * root)
    if 8 * step == 3 * denominator:
        root = math.sqrt(0.5)
        return ((im - re) * root, -(re + im) * root)
    c = math.cos(2 * math.pi * step / denominator)
    s = math.sin(2 * math.pi * step / denominator)
    return (re * c + im * s, im * c - re * s)


def transform16(values):
    inner = [quarter(values[n], values[4 + n], values[8 + n], values[12 + n]) for n in range(4)]
    out = [None] * 16
    for k1 in range(4):
        column = [turn(inner[n][k1], n * k1, 16) for n in range(4)]
        for k2, value in enumerate(quarter(*column)):
            out[k1 + 4 * k2] = value
    return out


def split(value):
    high = value.astype(BF16)
    return high, (value - high.astype(F32)).astype(BF16)


def dot(a, b, dims):
    return lax.dot_general(a, b, dims, preferred_element_type=F32)


def cosine_of_turns(steps, period):
    turns = steps * (1.0 / period)
    turns = turns - jnp.floor(turns)
    s = (0.25 - jnp.abs(turns - 0.5)) * (2.0 * math.pi)
    s2 = s * s
    poly = 1.0 / 6227020800.0
    for c in (-1.0 / 39916800.0, 1.0 / 362880.0, -1.0 / 5040.0, 1.0 / 120.0, -1.0 / 6.0, 1.0):
        poly = poly * s2 + c
    return -(poly * s)


def z_transform(levels, table, rows, ready, member):
    for half in range(2):
        high, low = split(levels[2 * member + half].reshape(256, 128).T)
        out = dot(high, table[0], NN) + dot(high, table[1], NN) + dot(low, table[0], NN)
        for k1 in range(16):
            for part in range(2):
                at = k1 * 32 + 16 * half + part
                rows[pl.ds(at, 8, stride=2), :] = out[8 * k1 : 8 * k1 + 8, 128 * part : 128 * part + 128]
    value = rows[...].reshape(16, 32, 128)
    for low_k in range(2):
        ready[pl.ds(low_k * 16, 16)] = value[:, :, low_k * NZ : (low_k + 1) * NZ]


def exchange_kernel(
    field, modes_in, x_tab, y_tab, y_twid, z_tab,
    levels_out, local_out, z_t, ready,
    cells, modes, x_t, y_t, tw, cells_parts, lines, blocks, y_parts, waves, phases, chosen, z_rows,
    coef_one, coef_mine, coef_col, coef_row, coef_sum, coef_all,
    load_sem, row_send, row_recv, col_send, col_recv,
    small_send, small_recv,
):
    row, col = lax.axis_index("row"), lax.axis_index("col")
    z_at, y_lo = lax.rem(row, 8), row // 8

    def row_peer(k):
        return lax.rem(z_at + k, 8) + 8 * lax.rem(y_lo + k // 8, 2)

    x_at, y_hi, core = col // 4, lax.rem(col // 2, 2), lax.rem(col, 2)

    def col_peer(k):
        x_step, y_step, core_step = (2, 1, 3, 0)[(k - 1) // 4], 1 - ((k - 1) // 2) % 2, k % 2
        return lax.rem(x_at + x_step, 4) * 4 + lax.rem(y_hi + y_step, 2) * 2 + lax.rem(core + core_step, 2)

    barrier = pltpu.get_barrier_semaphore()

    for z_step in (4, 3, 5, 2, 6, 1, 7, 0):
        for y_step in (1, 0):
            if z_step or y_step:
                peer = lax.rem(z_at + z_step, 8) + 8 * lax.rem(y_lo + y_step, 2)
                pl.semaphore_signal(barrier, inc=1, device_id={"row": peer}, device_id_type=MESH)
    for k in range(1, PEERS):
        pl.semaphore_signal(barrier, inc=1, device_id={"col": col_peer(k)}, device_id_type=MESH)

    pieces = [(x_tab, x_t)] + [(field.at[:, pl.ds(128 * t, 128)], cells.at[t]) for t in range(NX // 128)]
    first_pieces = len(pieces)
    pieces += [(modes_in, modes), (y_twid, tw), (y_tab, y_t), (z_tab, z_t)]
    loads = [pltpu.make_async_copy(source, target, load_sem.at[i]) for i, (source, target) in enumerate(pieces)]
    for each in loads:
        each.start()

    def row_copy(chunk, peer):
        return pltpu.make_async_remote_copy(
            src_ref=lines.at[chunk, peer], dst_ref=blocks.at[chunk, row],
            send_sem=row_send.at[chunk], recv_sem=row_recv.at[chunk],
            device_id={"row": peer}, device_id_type=MESH,
        )

    def col_copy(chunk, k):
        peer = col_peer(k)
        return pltpu.make_async_remote_copy(
            src_ref=waves.at[chunk, peer], dst_ref=levels_out.at[chunk, col],
            send_sem=col_send.at[chunk], recv_sem=col_recv.at[chunk],
            device_id={"col": peer}, device_id_type=MESH,
        )

    def wait_bytes(ref, sem):
        pltpu.make_async_copy(ref, ref, sem).wait()

    def send_rows(slot):
        for plane, lead in zip(PLANES, LEAD):
            chunk = slot + lead
            there = jnp.logical_and(chunk >= 0, chunk < CHUNKS)
            for peer in (plane + 8 * (1 - y_lo), plane + 8 * y_lo):

                @pl.when(jnp.logical_and(there, peer != row))
                def _(chunk=chunk, peer=peer):
                    row_copy(chunk, peer).start()

    for each in loads[:first_pieces]:
        each.wait()
    def x_transform(member):
        for t in range(NX // 128):
            high, low = split(cells[t, pl.ds(member, ROWS * LEVELS, stride=MEMBERS), :])
            lanes = pl.ds(t * 128, 128)
            cells_parts[pl.ds(0, 128), lanes], cells_parts[pl.ds(128, 128), lanes] = high, low
        for half in range(2):
            chunk = member * 2 + half
            table = pl.ds(half * 256, 256)
            both = dot(x_t[0, table], cells_parts[...], NT)
            value = both[:, :128] + both[:, 128:] + dot(x_t[1, table], cells_parts[pl.ds(0, 128)], NT)
            lines[chunk] = value.reshape(PEERS, 16, 128)
            blocks[chunk, row] = lines[chunk, row]

    x_transform(0)
    pl.semaphore_wait(barrier, 2 * (PEERS - 1))
    for slot in (-2, -1):
        send_rows(slot)

    @pl.loop(1, MEMBERS)
    def _(member):
        x_transform(member)

        @pl.when(member <= AHEAD // 2)
        def _():
            send_rows(2 * member - 2)
            send_rows(2 * member - 1)

    for each in loads[first_pieces:]:
        each.wait()

    def mode_row(i):
        return modes[i : i + 1, :].astype(F32)

    def down(value):
        return jnp.broadcast_to(value, (128, MODES)).T

    kx = mode_row(0)
    block = jnp.floor(kx * (1.0 / 16.0))
    half = jnp.floor((kx - 16.0 * block) * 0.125)
    place = half * 256.0 + block * 16.0 + (kx - 16.0 * block - 8.0 * half)
    place = down(place)
    lane = lax.broadcasted_iota(jnp.int32, (MODES, 128), 1)
    lane_f = lane.astype(F32)
    choose = jnp.concatenate(
        [
            jnp.concatenate([(place + 8.0 * part == lane_f + 128.0 * t).astype(F32) for t in range(4)], axis=1)
            for part in range(2)
        ],
        axis=0,
    ).astype(BF16)
    cell = (lane // 4).astype(F32) + (row * ROWS).astype(F32)
    level = lax.rem(lane, 4).astype(F32) + (col * LEVELS).astype(F32)
    steps = down(mode_row(1)) * cell + down(mode_row(2)) * level * float(NY // NZ)
    cos = cosine_of_turns(steps, float(NY))
    sin = cosine_of_turns(steps - 128.0, float(NY))
    phases[0], phases[1] = cos, sin
    chosen[...] = choose
    own_member = lax.broadcasted_iota(jnp.int32, (8, 128), 0)

    def add_member(member, coef):
        here = (own_member == member).astype(F32).astype(BF16)
        high, low = split(lines[pl.ds(2 * member, 2)].reshape(512, 128))
        both = dot(chosen[...], jnp.concatenate([high, low], axis=1), NN)
        at_modes = both[:, :128] + both[:, 128:]
        re, im = at_modes[:MODES], at_modes[MODES:]
        cos, sin = phases[0], phases[1]
        value = jnp.concatenate([re * cos + im * sin, im * cos - re * sin], axis=0)
        high, low = split(value)
        return coef + dot(here, high, NT) + dot(here, low, NT)

    coef = lax.fori_loop(0, MEMBERS, add_member, jnp.zeros((8, 2 * MODES), F32))
    for t in range(4):
        for pair in range(4):
            coef_one[4 * t + pair] = coef[2 * pair : 2 * pair + 2, 128 * t : 128 * t + 128]

    def piece_copy(k):
        peer = col_peer(k)
        return pltpu.make_async_remote_copy(
            src_ref=coef_one.at[peer], dst_ref=coef_col.at[col],
            send_sem=small_send.at[0], recv_sem=small_recv.at[0], device_id={"col": peer}, device_id_type=MESH,
        )

    def sum_copy(k):
        return pltpu.make_async_remote_copy(
            src_ref=coef_mine, dst_ref=coef_row.at[row],
            send_sem=small_send.at[1], recv_sem=small_recv.at[1], device_id={"row": row_peer(k)}, device_id_type=MESH,
        )

    def share_copy(k):
        return pltpu.make_async_remote_copy(
            src_ref=coef_sum, dst_ref=coef_all.at[col],
            send_sem=small_send.at[2], recv_sem=small_recv.at[2], device_id={"col": col_peer(k)}, device_id_type=MESH,
        )

    def start_all(copy):
        for k in range(1, PEERS):
            copy(k).start()

    coef_col[col] = coef_one[col]
    start_all(piece_copy)

    def small_step(step):
        if step == 0:
            wait_bytes(coef_col.at[pl.ds(0, PEERS - 1)], small_recv.at[0])
            total = coef_col[0]
            for i in range(1, PEERS):
                total = total + coef_col[i]
            coef_mine[...] = total
            coef_row[row] = total
            start_all(sum_copy)
        elif step == 1:
            wait_bytes(coef_row.at[pl.ds(0, PEERS - 1)], small_recv.at[1])
            total = coef_row[0]
            for i in range(1, PEERS):
                total = total + coef_row[i]
            coef_sum[...] = total
            coef_all[col] = total
            start_all(share_copy)
        else:
            wait_bytes(coef_all.at[pl.ds(0, PEERS - 1)], small_recv.at[2])
            tiles = [jnp.concatenate([coef_all[4 * t + pair] for pair in range(4)], axis=0) for t in range(4)]
            coef = jnp.concatenate(tiles, axis=1)
            anomaly = coef - jnp.mean(coef, axis=0, keepdims=True)
            turned = anomaly.T
            a_high, a_low = split(turned)
            b_high, b_low = split(anomaly)
            kx, ky, kz = mode_row(0), mode_row(1), mode_row(2)
            ky = jnp.where(ky < NY // 2, ky, ky - NY)
            kz = jnp.where(kz < NZ // 2, kz, kz - NZ)
            dist = jnp.zeros((MODES, MODES), F32)
            for wave in (kx, ky, kz):
                tall = down(wave)
                tall = jnp.concatenate([tall, tall], axis=1)
                dist += (tall - wave) ** 2
            taper = jnp.exp(-dist * (1.0 / (2.0 * REACH * REACH))) * (1.0 / (MEMBERS - 1))
            for i in range(2):
                at = slice(i * MODES, (i + 1) * MODES)
                cov = dot(a_high[at], b_high, NN) + dot(a_high[at], b_low, NN) + dot(a_low[at], b_high, NN)
                local_out[at, :MODES] = cov[:, :MODES] * taper
                local_out[at, MODES:] = cov[:, MODES:] * taper

    @pl.loop(0, CHUNKS)
    def _(chunk):
        send_rows(chunk + AHEAD)

        wait_bytes(blocks.at[chunk, pl.ds(0, PEERS - 1)], row_recv.at[chunk])
        out = transform16([(blocks[chunk, i, 0:8, :], blocks[chunk, i, 8:16, :]) for i in range(16)])
        for pair in range(8):
            parts = []
            for k1 in (2 * pair, 2 * pair + 1):
                re, im = out[k1]
                if k1 > 0:
                    c = tw[2 * k1 : 2 * k1 + 1, :]
                    s = tw[2 * k1 + 1 : 2 * k1 + 2, :]
                    re, im = re * c + im * s, im * c - re * s
                parts.append((re, im))
            for part in range(2):
                high, low = split(jnp.concatenate([parts[0][part], parts[1][part]], axis=0))
                at = pl.ds(part * 128, 128)
                y_parts[pl.ds(16 * pair, 16), at] = high
                y_parts[pl.ds(128 + 16 * pair, 16), at] = low
        both = dot(y_t[0], y_parts[...], NT)
        value = both[:, :128] + both[:, 128:] + dot(y_t[1], y_parts[pl.ds(0, 128)], NT)
        waves[chunk] = value.reshape(PEERS, 16, 128)

        for k in range(1, PEERS):
            col_copy(chunk, k).start()

        levels_out[chunk, col] = waves[chunk, col]

        for step, at in enumerate((4, 9)):
            @pl.when(chunk == at)
            def _(step=step):
                small_step(step)

    small_step(2)

    def wait_levels(member):
        for chunk in (2 * member, 2 * member + 1):
            wait_bytes(levels_out.at[chunk, pl.ds(0, PEERS - 1)], col_recv.at[chunk])

    @pl.loop(0, DONE)
    def _(member):
        wait_levels(member)
        z_transform(levels_out, z_t, z_rows, ready.at[member], member)

    for member in range(DONE, MEMBERS):
        wait_levels(member)
    wait_bytes(coef_col.at[pl.ds(0, PEERS - 1)], small_send.at[0])
    wait_bytes(coef_row.at[pl.ds(0, PEERS - 1)], small_send.at[1])
    wait_bytes(coef_all.at[pl.ds(0, PEERS - 1)], small_send.at[2])

    @pl.loop(0, CHUNKS)
    def _(chunk):
        wait_bytes(lines.at[chunk, pl.ds(0, PEERS - 1)], row_send.at[chunk])
        wait_bytes(waves.at[chunk, pl.ds(0, PEERS - 1)], col_send.at[chunk])


def exchange(field, modes):
    any_space = pl.BlockSpec(memory_space=pl.ANY)
    dma = pltpu.SemaphoreType.DMA
    return pl.pallas_call(
        exchange_kernel,
        out_shape=(
            pltpu.VMEM((CHUNKS, PEERS, 16, 128), F32),
            pltpu.VMEM((2 * MODES, 2 * MODES), F32),
            pltpu.VMEM((2, 256, 256), BF16),
            pltpu.VMEM((MEMBERS, NY // PEERS, 32, NZ), F32),
        ),
        in_specs=[any_space] * 6,
        out_specs=(pl.BlockSpec(memory_space=pltpu.VMEM),) * 4,
        scratch_shapes=[
            pltpu.VMEM((NX // 128, ROWS * LEVELS * MEMBERS, 128), F32),
            pltpu.VMEM((3, MODES), jnp.int32),
            pltpu.VMEM((2, 512, 512), BF16),
            pltpu.VMEM((2, 256, 256), BF16),
            pltpu.VMEM((32, 128), F32),
            pltpu.VMEM((256, NX), BF16),
            pltpu.VMEM((CHUNKS, PEERS, 16, 128), F32),
            pltpu.VMEM((CHUNKS, PEERS, 16, 128), F32),
            pltpu.VMEM((256, 256), BF16),
            pltpu.VMEM((CHUNKS, PEERS, 16, 128), F32),
            pltpu.VMEM((2, MODES, 128), F32),
            pltpu.VMEM((512, 512), BF16),
            pltpu.VMEM((512, 128), F32),
            pltpu.VMEM((PEERS, 2, 128), F32),
            pltpu.VMEM((2, 128), F32),
            pltpu.VMEM((PEERS, 2, 128), F32),
            pltpu.VMEM((PEERS, 2, 128), F32),
            pltpu.VMEM((2, 128), F32),
            pltpu.VMEM((PEERS, 2, 128), F32),
            dma((9,)),
            dma((CHUNKS,)),
            dma((CHUNKS,)),
            dma((CHUNKS,)),
            dma((CHUNKS,)),
            dma((3,)),
            dma((3,)),
        ],
        compiler_params=pltpu.CompilerParams(collective_id=0, has_side_effects=True, vmem_limit_bytes=VMEM),
        cost_estimate=pl.CostEstimate(flops=10**10, bytes_accessed=8 << 20, transcendentals=0),
        name="exchange",
    )(field.reshape(-1, NX), modes, x_table(), y_table(), y_twiddle(), z_table())


def levels_kernel(levels, local_in, table, ready, spectrum, local, rows, last, out_sem, local_sem):
    copies = [pltpu.make_async_copy(local_in, local, local_sem)]
    for member in range(MEMBERS):
        source = ready.at[member] if member < DONE else last.at[member - DONE]
        copies.append(pltpu.make_async_copy(source, spectrum.at[:, member], out_sem.at[member]))
    for copy in copies[1 : DONE + 1]:
        copy.start()
    copies[0].start()
    for member in range(DONE, MEMBERS):
        z_transform(levels, table, rows, last.at[member - DONE], member)
        copies[member + 1].start()
    for copy in copies:
        copy.wait()


def from_levels(*parts):
    here = pl.BlockSpec(memory_space=pltpu.VMEM)
    any_space = pl.BlockSpec(memory_space=pl.ANY)
    spectrum, local = pl.pallas_call(
        levels_kernel,
        out_shape=(
            jax.ShapeDtypeStruct((NY // PEERS, MEMBERS, 32, NZ), F32),
            jax.ShapeDtypeStruct((2 * MODES, 2 * MODES), F32),
        ),
        in_specs=[here] * 4,
        out_specs=(any_space, any_space),
        scratch_shapes=[
            pltpu.VMEM((512, 128), F32),
            pltpu.VMEM((MEMBERS - DONE, NY // PEERS, 32, NZ), F32),
            pltpu.SemaphoreType.DMA((MEMBERS,)),
            pltpu.SemaphoreType.DMA,
        ],
        compiler_params=pltpu.CompilerParams(vmem_limit_bytes=VMEM),
        cost_estimate=pl.CostEstimate(flops=10**9, bytes_accessed=8 << 20, transcendentals=0),
        name="from_levels",
    )(*(pltpu.with_memory_space_constraint(each, pltpu.VMEM) for each in parts))
    return jnp.transpose(spectrum, (3, 0, 1, 2)), local


def per_device(field, modes):
    return from_levels(*exchange(field, modes))


def solution(mesh):
    return jax.shard_map(
        per_device,
        mesh=mesh,
        in_specs=(P("row", "col", None, None), P()),
        out_specs=(P(None, "col", None, "row"), P()),
        check_vma=False,
    )
```
